8 devices in a mesh: part: 1 (over z), col: 2 (over y), row: 4 (over x, core).
Axes of the slice: x: 2, y: 2, z: 1, core: 2. Of those that a mesh axis runs over, the one named last changes fastest.
Arguments:
- a_blocks: float32 [128, 64, 8192], P(('part', 'row'), None, 'col')
Outputs:
- output: float32 [128, 64, 8192], P(('part', 'row'), None, 'col')
All inputs are finite; a program needn't handle non-finite values.
Results may differ from the reference program's by a relative error of at most 0.001.
Values sent between devices are 32-bit elements.
A program may use at most 1 GiB of HBM per device.

```python
import jax
import jax.numpy as jnp

N = 8192
NB = 64
GRID_ROWS = 4
GRID_COLS = 2
NUM_BLOCKS = N // NB
ROW_BLOCKS = NUM_BLOCKS // GRID_ROWS
COL_BLOCKS = NUM_BLOCKS // GRID_COLS
RANK_COLS = N // 4


def to_natural(blocked):
    row_perm = blocked.reshape(GRID_ROWS, ROW_BLOCKS, NB, N).transpose(1, 0, 2, 3).reshape(N, N)
    return row_perm.reshape(N, GRID_COLS, COL_BLOCKS, NB).transpose(0, 2, 1, 3).reshape(N, N)


def to_cyclic(matrix):
    row_perm = matrix.reshape(ROW_BLOCKS, GRID_ROWS, NB, N).transpose(1, 0, 2, 3).reshape(N, N)
    return row_perm.reshape(N, COL_BLOCKS, GRID_COLS, NB).transpose(0, 2, 1, 3).reshape(NUM_BLOCKS, NB, N)


def setup_inputs(seed: int = 0, part: int = 0) -> dict:
    base_key = jax.random.fold_in(jax.random.key(seed), part)
    factor = jax.random.normal(base_key, (N, RANK_COLS), jnp.float32)
    gram_mat = jnp.dot(factor, factor.T, preferred_element_type=jnp.float32)
    spd_matrix = 0.5 * (gram_mat + gram_mat.T) / RANK_COLS + jnp.eye(N, dtype=jnp.float32)
    return {"a_blocks": to_cyclic(spd_matrix)}


def reference(a_blocks):
    lower = jnp.linalg.cholesky(to_natural(a_blocks))
    return to_cyclic(lower)
```

```python
import jax
import jax.numpy as jnp
from jax import lax
from jax.experimental import pallas as pl
from jax.experimental.pallas import tpu as pltpu
from jax.sharding import PartitionSpec as P

F32 = jnp.float32
FULL = lax.Precision.HIGHEST
SB = 256
TR = 64
TC = 128
LANES = 128
GROUP = 8
CHUNK = 32
QS = 4
ORDER = (0, 2, 1, 3)


def _nn(a, b):
    return lax.dot_general(a, b, (((1,), (0,)), ((), ())), precision=FULL, preferred_element_type=F32)


def _nt(a, b):
    return lax.dot_general(a, b, (((1,), (1,)), ((), ())), precision=FULL, preferred_element_type=F32)


def _swap_middle(x0, x1):
    low = lax.broadcasted_iota(jnp.int32, x0.shape, 1) < LANES // 2
    half = LANES // 2
    return jnp.where(low, x0, pltpu.roll(x1, half, 1)), jnp.where(low, pltpu.roll(x0, half, 1), x1)


def _factor128(src):
    size = LANES
    lane = lax.broadcasted_iota(jnp.int32, (size, LANES), 1)
    rows = lax.broadcasted_iota(jnp.int32, (size, LANES), 0)
    left = src
    right = jnp.where(lane == rows, 1.0, 0.0).astype(F32)
    rid = lax.broadcasted_iota(jnp.int32, (GROUP, LANES), 0)
    lid = lax.broadcasted_iota(jnp.int32, (GROUP, LANES), 1)
    upper, inverse = [], []
    for g in range(size // GROUP):
        base = GROUP * g
        top_l, top_r = left[:GROUP], right[:GROUP]
        cols = [jnp.broadcast_to(top_l[:, base + j : base + j + 1], (GROUP, LANES)) for j in range(GROUP)]
        scale, row_l, row_r, mult = [], [], [], {}
        for j in range(GROUP):
            inv = lax.rsqrt(cols[j][j : j + 1])
            low = jnp.where(rid > j, cols[j] * inv, 0.0)
            u_l, u_r = top_l[j : j + 1] * inv, top_r[j : j + 1] * inv
            for k in range(j + 1, GROUP):
                mult[j, k] = cols[k][j : j + 1] * inv
                cols[k] = cols[k] - low * mult[j, k]
            top_l = jnp.where(rid == j, u_l, top_l - low * u_l)
            top_r = jnp.where(rid == j, u_r, top_r - low * u_r)
            scale.append(inv)
            row_l.append(u_l)
            row_r.append(u_r)
        upper.append(jnp.where(lid >= rid + base, top_l, 0.0))
        inverse.append(top_r)
        rest = size - base - GROUP
        if rest == 0:
            break
        next_l, next_r = [], []
        for start in range(0, rest, CHUNK):
            stop = min(start + CHUNK, rest)
            a, b = left[GROUP + start : GROUP + stop], right[GROUP + start : GROUP + stop]
            below = [jnp.broadcast_to(a[:, base + j : base + j + 1], (stop - start, LANES)) for j in range(GROUP)]
            for j in range(GROUP):
                low = below[j] * scale[j]
                for k in range(j + 1, GROUP):
                    below[k] = below[k] - low * mult[j, k]
                a = a - low * row_l[j]
                b = b - low * row_r[j]
            next_l.append(a)
            next_r.append(b)
        left = jnp.concatenate(next_l, 0) if len(next_l) > 1 else next_l[0]
        right = jnp.concatenate(next_r, 0) if len(next_r) > 1 else next_r[0]
    return upper, inverse


def _kernel(steps, a_hbm, out_hbm, mat, left, right, xl, xrt, pieces, diag, upper, lower, inv, invp, a1, zeros,
            load_sem, out_sem, sg_send, sg_recv, fw_send, fw_recv, f1_send, f1_recv, f2_send, f2_recv, f3_send, f3_recv):
    r = lax.axis_index("row")
    c = lax.axis_index("col")
    x = r // 2
    p = r % 2
    me = r * 2 + c
    major = p == c
    chunks = steps // QS
    rows, cols = steps * TR, steps * TC
    own = pl.multiple_of(c * TC, TC)
    other = pl.multiple_of((1 - c) * TC, TC)
    y_peer = {"row": r, "col": 1 - c}
    x_peer = {"row": (r + 2) % 4, "col": c}
    z_peer = {"row": (r + 2) % 4, "col": 1 - c}
    d_peer = {"row": 2 * x + 1 - p, "col": c}
    peers = (d_peer, y_peer, x_peer, z_peer)
    xi = (r + 2) % 4

    def small(par, i):
        return pltpu.make_async_remote_copy(pieces.at[par, me], pieces.at[par, me], sg_send.at[par, i],
                                            sg_recv.at[par, i], device_id=peers[i])

    sources = (None, r * 2 + 1 - c, xi * 2 + c, xi * 2 + 1 - c)

    def forward(par, i):
        return pltpu.make_async_remote_copy(pieces.at[par, sources[i]], pieces.at[par, sources[i]], fw_send.at[par, i - 1],
                                            fw_recv.at[par, i - 1], device_id=d_peer)

    def start_small(par):
        for i in range(4):
            small(par, i).start()

    def forward_small(par):
        for i in range(1, 4):
            small(par, i).wait_recv()
            forward(par, i).start()

    def finish_small(par):
        small(par, 0).wait_recv()
        for i in range(1, 4):
            forward(par, i).wait_recv()
        for i in range(4):
            small(par, i).wait_send()
        for i in range(1, 4):
            forward(par, i).wait_send()

    def f1(par, q):
        ref = left.at[par, pl.ds(QS * q, QS), :, pl.ds(own, TC)]
        return pltpu.make_async_remote_copy(ref, ref, f1_send.at[par, q], f1_recv.at[par, q], device_id=y_peer)

    def f2(par, q, h, at):
        return pltpu.make_async_remote_copy(left.at[par, pl.ds(QS * q, QS), :, pl.ds(at, TC)],
                                            right.at[par, pl.ds(QS * q, QS), x, :, pl.ds(at, TC)],
                                            f2_send.at[par, q, h], f2_recv.at[par, q, h], device_id=x_peer)

    def f3a(par, q):
        return pltpu.make_async_remote_copy(left.at[par, pl.ds(QS * q, QS)], right.at[par, pl.ds(QS * q, QS), x],
                                            f3_send.at[par, q, 0], f3_recv.at[par, q, 0], device_id=d_peer)

    def f3b(par, q):
        ref = right.at[par, pl.ds(QS * q, QS), 1 - x]
        return pltpu.make_async_remote_copy(ref, ref, f3_send.at[par, q, 1], f3_recv.at[par, q, 1], device_id=d_peer)

    def rows_of(q):
        return pl.ds(pl.multiple_of(QS * TR * q, QS * TR), QS * TR)

    def cols_of(k, n=1):
        return pl.ds(pl.multiple_of(TC * k, TC), n * TC)

    def each(lo, hi, body):
        def step(i, carry):
            body(i)
            return carry

        lax.fori_loop(lo, hi, step, 0)

    def load(q):
        return pltpu.make_async_copy(a_hbm.at[rows_of(q)], mat.at[rows_of(q)], load_sem.at[q])

    each(0, chunks, lambda q: load(q).start())
    zeros[...] = jnp.zeros_like(zeros)

    def clear(q):
        xl[rows_of(q), :] = jnp.zeros((QS * TR, SB), F32)
        xrt[:, cols_of(QS * q, QS)] = jnp.zeros((SB, QS * TC), F32)

    each(0, chunks, clear)
    each(0, chunks, lambda q: load(q).wait())

    def place_diag(par):
        for i in range(4):
            s0, s1 = _swap_middle(pieces[par, 2 * i, TR:, :], pieces[par, 2 * i + 1, TR:, :])
            diag[TR * i : TR * i + TR, :LANES] = s0
            diag[TR * i : TR * i + TR, LANES:] = s1

    pieces[1, me] = jnp.zeros((2 * TR, TC), F32)
    pieces[1, me, TR:, :] = mat[:TR, :TC]
    start_small(1)
    forward_small(1)
    finish_small(1)
    place_diag(1)

    def relay_one(par, q0):
        def body(q):
            f1(par, q).wait_recv()

            @pl.when(major)
            def _():
                f2(par, q, 1, other).start()
                f3a(par, q).start()
                right[par, pl.ds(QS * q, QS), x] = left[par, pl.ds(QS * q, QS)]

        each(q0, chunks, body)

    def relay_two(par, q0):
        @pl.when(major)
        def _():
            def body(q):
                f2(par, q, 0, own).wait_recv()
                f2(par, q, 1, other).wait_recv()
                f3b(par, q).start()

            each(q0, chunks, body)

    def bulk(k, lo, hi):
        def row_tile(t):
            def tile(u):
                rs = pl.ds(pl.multiple_of(512 * t, 512), 512)
                cs = pl.ds(pl.multiple_of(512 * u, 512), 512)
                mat[rs, cs] = mat[rs, cs] - _nn(xl[rs, :], xrt[:, cs])

            each((k + 2) // 4, 2 * t + 2, tile)

        each(lo, hi, row_tile)

    def step(k, carry):
        par = k % 2
        q0 = k // QS
        more = k < steps - 1
        early = k < steps // 2

        @pl.when(more)
        def _():
            nxt = pl.ds(pl.multiple_of(TR * (k + 1), TR), TR)
            pieces[par, me, :TR, :] = mat[nxt, cols_of(k)]
            pieces[par, me, TR:, :] = mat[nxt, cols_of(k + 1)]
            start_small(par)

            def send(q):
                left[par, pl.ds(QS * q, QS), :, pl.ds(own, TC)] = mat[rows_of(q), cols_of(k)].reshape(QS, TR, TC)
                f1(par, q).start()

                @pl.when(major)
                def _():
                    f2(par, q, 0, own).start()

            each(q0, chunks, send)

        tiles = rows // 512
        first = (k + 2) // 8

        @pl.when(k > 0)
        def _():
            bulk(k, jnp.maximum(first, tiles - 1), tiles)

        @pl.when(more & early)
        def _():
            relay_one(par, q0)

        @pl.when(k > 0)
        def _():
            bulk(k, first, tiles - 1)

        def factor(at):
            u, w = _factor128(diag[at : at + LANES, at : at + LANES])
            for i in range(LANES // GROUP):
                upper[GROUP * i : GROUP * i + GROUP, :] = u[i]
                inv[at + GROUP * i : at + GROUP * i + GROUP, at : at + LANES] = w[i]
            lower[at : at + LANES, at : at + LANES] = upper[...].T

        factor(0)

        @pl.when(more & early)
        def _():
            relay_two(par, q0)

        @pl.when(more & jnp.logical_not(early))
        def _():
            relay_one(par, q0)

        @pl.when(more)
        def _():
            forward_small(par)

        w00 = inv[:LANES, :LANES]
        l10 = _nt(diag[LANES:, :LANES], w00)
        lower[LANES:, :LANES] = l10
        lower[:LANES, LANES:] = jnp.zeros((LANES, LANES), F32)
        diag[LANES:, LANES:] = diag[LANES:, LANES:] - _nt(l10, l10)
        factor(LANES)

        @pl.when(more & jnp.logical_not(early))
        def _():
            relay_two(par, q0)

        inv[LANES:, :LANES] = -_nn(inv[LANES:, LANES:], _nn(l10, w00))
        inv[:LANES, LANES:] = jnp.zeros((LANES, LANES), F32)
        for i in range(4):
            s0, s1 = _swap_middle(inv[TR * ORDER[i] : TR * ORDER[i] + TR, :LANES], inv[TR * ORDER[i] : TR * ORDER[i] + TR, LANES:])
            invp[TR * i : TR * i + TR, :LANES] = s0
            invp[TR * i : TR * i + TR, LANES:] = s1

        @pl.when(more)
        def _():
            finish_small(par)
            for i in range(4):
                a1[TR * i : TR * i + TR, :LANES] = pieces[par, 2 * i, :TR, :]
                a1[TR * i : TR * i + TR, LANES:] = pieces[par, 2 * i + 1, :TR, :]
            place_diag(par)
            x1 = _nt(a1[...], invp[...])
            diag[...] = diag[...] - _nt(x1, x1)

        def put(q):
            return pltpu.make_async_copy(xl.at[rows_of(q), pl.ds(own, TC)], out_hbm.at[rows_of(q), cols_of(k)], out_sem.at[q])

        def put_zero(q, at):
            return pltpu.make_async_copy(zeros, out_hbm.at[rows_of(q), cols_of(at)], out_sem.at[q])

        @pl.when(k > 0)
        def _():
            each(0, chunks, lambda q: put_zero(q, k - 1).wait())

        @pl.when(more)
        def _():
            @pl.when(jnp.logical_not(major))
            def _():
                def body(q):
                    f3a(par, q).wait_recv()
                    f3b(par, q).wait_recv()

                each(q0, chunks, body)

            def solve(q):
                xl[rows_of(q), :] = _nt(left[par, pl.ds(QS * q, QS)].reshape(QS * TR, SB), invp[...])
                xrt[:, cols_of(QS * q, QS)] = _nt(invp[...], right[par, pl.ds(QS * q, QS)].reshape(2 * QS * TR, SB))

            each(q0, chunks, solve)

        def clear_above(i):
            xl[pl.ds(pl.multiple_of(TR * i, TR), TR), :] = jnp.zeros((TR, SB), F32)

        each(QS * q0, k, clear_above)
        mine = pl.ds(pl.multiple_of(TR * r, TR), TR)
        s0, s1 = _swap_middle(lower[mine, :LANES], lower[mine, LANES:])
        at = pl.ds(pl.multiple_of(TR * k, TR), TR)
        xl[at, :LANES] = s0
        xl[at, LANES:] = s1
        each(0, q0, lambda q: put_zero(q, k).start())
        each(q0, chunks, lambda q: put(q).start())

        @pl.when(more)
        def _():
            cs = pl.ds(pl.multiple_of(TC * jnp.minimum(k + 1, steps - 2), TC), 2 * TC)

            def update(q):
                mat[rows_of(q), cs] = mat[rows_of(q), cs] - _nn(xl[rows_of(q), :], xrt[:, cs])

            each((k + 1) // QS, chunks, update)
            xrt[:, cs] = jnp.zeros((SB, 2 * TC), F32)

            def sent(q):
                f1(par, q).wait_send()

                @pl.when(major)
                def _():
                    f2(par, q, 0, own).wait_send()
                    f2(par, q, 1, other).wait_send()
                    f3a(par, q).wait_send()
                    f3b(par, q).wait_send()

            each(q0, chunks, sent)

        return carry

    lax.fori_loop(0, steps, step, 0)
    each(0, chunks, lambda q: pltpu.make_async_copy(zeros, out_hbm.at[rows_of(q), cols_of(steps - 1)], out_sem.at[q]).wait())


def solution(mesh):
    def local_factor(blocks):
        row_blocks, block_size, local_cols = blocks.shape
        rows = row_blocks * block_size
        steps = local_cols // TC
        chunks = steps // QS
        dma = pltpu.SemaphoreType.DMA
        vm = lambda *s: pltpu.VMEM(s, F32)
        out = pl.pallas_call(
            lambda *refs: _kernel(steps, *refs),
            out_shape=jax.ShapeDtypeStruct((rows, local_cols), F32),
            in_specs=[pl.BlockSpec(memory_space=pl.ANY)],
            out_specs=pl.BlockSpec(memory_space=pl.ANY),
            scratch_shapes=[
                vm(rows, local_cols),
                vm(2, steps, TR, SB),
                vm(2, steps, 2, TR, SB),
                vm(rows, SB),
                vm(SB, local_cols),
                vm(2, 8, 2 * TR, TC),
                vm(SB, SB),
                vm(LANES, LANES),
                vm(SB, SB),
                vm(SB, SB),
                vm(SB, SB),
                vm(SB, SB),
                vm(QS * TR, TC),
                dma((chunks,)),
                dma((chunks,)),
                dma((2, 4)),
                dma((2, 4)),
                dma((2, 3)),
                dma((2, 3)),
                dma((2, chunks)),
                dma((2, chunks)),
                dma((2, chunks, 2)),
                dma((2, chunks, 2)),
                dma((2, chunks, 2)),
                dma((2, chunks, 2)),
            ],
            compiler_params=pltpu.CompilerParams(has_side_effects=True, vmem_limit_bytes=67043328),
            name="cholesky",
        )(blocks.reshape(rows, local_cols))
        return out.reshape(row_blocks, block_size, local_cols)

    spec = P(("part", "row"), None, "col")
    return jax.shard_map(local_factor, mesh=mesh, in_specs=(spec,), out_specs=spec, check_vma=False)
```

```python
import jax
import jax.numpy as jnp
from jax import lax
from jax.experimental import pallas as pl
from jax.experimental.pallas import tpu as pltpu
from jax.sharding import PartitionSpec as P

F32 = jnp.float32
FULL = lax.Precision.HIGHEST
SB = 256
TR = 64
TC = 128
LANES = 128
GROUP = 8
CHUNK = 32
QS = 4
WS = 2
TILE = 512
ORDER = (0, 2, 1, 3)


def _nn(a, b):
    return lax.dot_general(a, b, (((1,), (0,)), ((), ())), precision=FULL, preferred_element_type=F32)


def _nt(a, b):
    return lax.dot_general(a, b, (((1,), (1,)), ((), ())), precision=FULL, preferred_element_type=F32)


def _swap_middle(x0, x1):
    low = lax.broadcasted_iota(jnp.int32, x0.shape, 1) < LANES // 2
    half = LANES // 2
    return jnp.where(low, x0, pltpu.roll(x1, half, 1)), jnp.where(low, pltpu.roll(x0, half, 1), x1)


def _factor128(src):
    size = LANES
    lane = lax.broadcasted_iota(jnp.int32, (size, LANES), 1)
    rows = lax.broadcasted_iota(jnp.int32, (size, LANES), 0)
    left = src
    right = jnp.where(lane == rows, 1.0, 0.0).astype(F32)
    rid = lax.broadcasted_iota(jnp.int32, (GROUP, LANES), 0)
    lid = lax.broadcasted_iota(jnp.int32, (GROUP, LANES), 1)
    upper, inverse = [], []
    for g in range(size // GROUP):
        base = GROUP * g
        top_l, top_r = left[:GROUP], right[:GROUP]
        cols = [jnp.broadcast_to(top_l[:, base + j : base + j + 1], (GROUP, LANES)) for j in range(GROUP)]
        scale, row_l, row_r, mult = [], [], [], {}
        for j in range(GROUP):
            inv = lax.rsqrt(cols[j][j : j + 1])
            low = jnp.where(rid > j, cols[j] * inv, 0.0)
            u_l, u_r = top_l[j : j + 1] * inv, top_r[j : j + 1] * inv
            for k in range(j + 1, GROUP):
                mult[j, k] = cols[k][j : j + 1] * inv
                cols[k] = cols[k] - low * mult[j, k]
            top_l = jnp.where(rid == j, u_l, top_l - low * u_l)
            top_r = jnp.where(rid == j, u_r, top_r - low * u_r)
            scale.append(inv)
            row_l.append(u_l)
            row_r.append(u_r)
        upper.append(jnp.where(lid >= rid + base, top_l, 0.0))
        inverse.append(top_r)
        rest = size - base - GROUP
        if rest == 0:
            break
        next_l, next_r = [], []
        for start in range(0, rest, CHUNK):
            stop = min(start + CHUNK, rest)
            a, b = left[GROUP + start : GROUP + stop], right[GROUP + start : GROUP + stop]
            below = [jnp.broadcast_to(a[:, base + j : base + j + 1], (stop - start, LANES)) for j in range(GROUP)]
            for j in range(GROUP):
                low = below[j] * scale[j]
                for k in range(j + 1, GROUP):
                    below[k] = below[k] - low * mult[j, k]
                a = a - low * row_l[j]
                b = b - low * row_r[j]
            next_l.append(a)
            next_r.append(b)
        left = jnp.concatenate(next_l, 0) if len(next_l) > 1 else next_l[0]
        right = jnp.concatenate(next_r, 0) if len(next_r) > 1 else next_r[0]
    return upper, inverse


def _kernel(steps, a_hbm, out_hbm, mat, left, right, xl, xrt, pieces, diag, upper, lower, inv, invp, a1, zeros,
            load_sem, out_sem, sg_send, sg_recv, fw_send, fw_recv, f1_send, f1_recv, f2_send, f2_recv, f3_send, f3_recv):
    r = lax.axis_index("row")
    c = lax.axis_index("col")
    x = r // 2
    p = r % 2
    me = r * 2 + c
    major = p == c
    chunks = steps // QS
    parts = steps // WS
    rows, cols = steps * TR, steps * TC
    tiles = rows // TILE
    own = pl.multiple_of(c * TC, TC)
    other = pl.multiple_of((1 - c) * TC, TC)
    xi = (r + 2) % 4
    y_peer = {"row": r, "col": 1 - c}
    x_peer = {"row": xi, "col": c}
    z_peer = {"row": xi, "col": 1 - c}
    d_peer = {"row": 2 * x + 1 - p, "col": c}
    peers = (d_peer, y_peer, x_peer, z_peer)

    def small(par, i):
        return pltpu.make_async_remote_copy(pieces.at[par, me], pieces.at[par, me], sg_send.at[par, i],
                                            sg_recv.at[par, i], device_id=peers[i])

    sources = (None, r * 2 + 1 - c, xi * 2 + c, xi * 2 + 1 - c)

    def forward(par, i):
        return pltpu.make_async_remote_copy(pieces.at[par, sources[i]], pieces.at[par, sources[i]], fw_send.at[par, i - 1],
                                            fw_recv.at[par, i - 1], device_id=d_peer)

    def start_small(par):
        for i in range(4):
            small(par, i).start()

    def forward_small(par):
        for i in range(1, 4):
            small(par, i).wait_recv()
            forward(par, i).start()

    def finish_small(par):
        small(par, 0).wait_recv()
        for i in range(1, 4):
            forward(par, i).wait_recv()
        for i in range(4):
            small(par, i).wait_send()
        for i in range(1, 4):
            forward(par, i).wait_send()

    def f1(par, w):
        ref = left.at[par, pl.ds(WS * w, WS), :, pl.ds(own, TC)]
        return pltpu.make_async_remote_copy(ref, ref, f1_send.at[par, w], f1_recv.at[par, w], device_id=y_peer)

    def f2(par, w, h, at):
        return pltpu.make_async_remote_copy(left.at[par, pl.ds(WS * w, WS), :, pl.ds(at, TC)],
                                            right.at[par, pl.ds(WS * w, WS), x, :, pl.ds(at, TC)],
                                            f2_send.at[par, w, h], f2_recv.at[par, w, h], device_id=x_peer)

    def f3a(par, w):
        return pltpu.make_async_remote_copy(left.at[par, pl.ds(WS * w, WS)], right.at[par, pl.ds(WS * w, WS), x],
                                            f3_send.at[par, w, 0], f3_recv.at[par, w, 0], device_id=d_peer)

    def f3b(par, w):
        ref = right.at[par, pl.ds(WS * w, WS), 1 - x]
        return pltpu.make_async_remote_copy(ref, ref, f3_send.at[par, w, 1], f3_recv.at[par, w, 1], device_id=d_peer)

    def relay_one(par, w):
        f1(par, w).wait_recv()

        @pl.when(major)
        def _():
            f2(par, w, 1, other).start()
            f3a(par, w).start()
            right[par, pl.ds(WS * w, WS), x] = left[par, pl.ds(WS * w, WS)]

    def relay_two(par, w):
        @pl.when(major)
        def _():
            f2(par, w, 0, own).wait_recv()
            f2(par, w, 1, other).wait_recv()
            f3b(par, w).start()

        @pl.when(jnp.logical_not(major))
        def _():
            f3a(par, w).wait_recv()
            f3b(par, w).wait_recv()

    def sent(par, w):
        f1(par, w).wait_send()

        @pl.when(major)
        def _():
            f2(par, w, 0, own).wait_send()
            f2(par, w, 1, other).wait_send()
            f3a(par, w).wait_send()
            f3b(par, w).wait_send()

    def rows_of(q):
        return pl.ds(pl.multiple_of(QS * TR * q, QS * TR), QS * TR)

    def cols_of(k, n=1):
        return pl.ds(pl.multiple_of(TC * k, TC), n * TC)

    def each(lo, hi, body):
        def step(i, carry):
            body(i)
            return carry

        lax.fori_loop(lo, hi, step, 0)

    head = min(3 * TC, cols)

    def load_head():
        return pltpu.make_async_copy(a_hbm.at[:, pl.ds(0, head)], mat.at[:, pl.ds(0, head)], load_sem.at[chunks])

    def load_rest(q):
        wide = min((QS * TC) * (q + 2), cols) - head
        at = (pl.ds(QS * TR * q, QS * TR), pl.ds(head, wide))
        return pltpu.make_async_copy(a_hbm.at[at], mat.at[at], load_sem.at[q])

    load_head().start()
    for q in range(chunks):
        load_rest(q).start()
    zeros[...] = jnp.zeros_like(zeros)
    load_head().wait()

    def place_diag(par):
        for i in range(4):
            s0, s1 = _swap_middle(pieces[par, 2 * i, TR:, :], pieces[par, 2 * i + 1, TR:, :])
            diag[TR * i : TR * i + TR, :LANES] = s0
            diag[TR * i : TR * i + TR, LANES:] = s1

    pieces[1, me] = jnp.zeros((2 * TR, TC), F32)
    pieces[1, me, TR:, :] = mat[:TR, :TC]
    start_small(1)
    forward_small(1)
    finish_small(1)
    place_diag(1)

    def step(k, carry):
        par = k % 2
        now = k % 3
        last = (k + 2) % 3
        q0 = k // QS
        w0 = (k + 1) // WS
        more = k < steps - 1
        pair = jnp.minimum(k + 1, steps - 2)

        u0 = (k + 2) // QS
        count = 0
        for t in range(tiles):
            count = count + jnp.maximum(2 * t + 2 - u0, 0)
        count = jnp.where(k > 0, count, 0)

        def tile(i):
            t, first, total = 0, 0, 0
            for s in range(tiles):
                total = total + jnp.maximum(2 * s + 2 - u0, 0)
                past = i >= total
                t = t + jnp.where(past, 1, 0)
                first = jnp.where(past, total, first)
            live = i < count
            t = jnp.where(live, t, 0)
            u = jnp.where(live, u0 + i - first, 2 * tiles - 1)
            rs = pl.ds(pl.multiple_of(TILE * t, TILE), TILE)
            cs = pl.ds(pl.multiple_of(TILE * u, TILE), TILE)
            mat[rs, cs] = mat[rs, cs] - _nn(xl[rs, :], xrt[:, cs])

        @pl.when(more)
        def _():
            nxt = pl.ds(pl.multiple_of(TR * (k + 1), TR), TR)
            pieces[par, me, :TR, :] = mat[nxt, cols_of(k)]
            pieces[par, me, TR:, :] = mat[nxt, cols_of(k + 1)]

            def send(w):
                at = pl.ds(pl.multiple_of(WS * TR * w, WS * TR), WS * TR)
                left[now, pl.ds(WS * w, WS), :, pl.ds(own, TC)] = mat[at, cols_of(k)].reshape(WS, TR, TC)
                f1(now, w).start()

                @pl.when(major)
                def _():
                    f2(now, w, 0, own).start()

            send(w0)
            start_small(par)
            each(w0 + 1, parts, send)

        @pl.when(k > 0)
        def _():
            each((k + 1) // WS + 1, parts, lambda w: relay_two(last, w))

            def solve_right(q):
                xrt[:, cols_of(QS * q, QS)] = _nt(invp[1 - par], right[last, pl.ds(QS * q, QS)].reshape(2 * QS * TR, SB))

            each(u0, chunks, solve_right)
            xrt[:, cols_of(jnp.minimum(k, steps - 2), 2)] = jnp.zeros((SB, 2 * TC), F32)

        @pl.when(k == 1)
        def _():
            for q in range(chunks):
                load_rest(q).wait()

        def chain(n):
            def half(h):
                @pl.when(h == 1)
                def _():
                    w00 = inv[:LANES, :LANES]
                    l10 = _nt(diag[LANES:, :LANES], w00)
                    lower[LANES:, :LANES] = l10
                    diag[LANES:, LANES:] = diag[LANES:, LANES:] - _nt(l10, l10)

                span = pl.ds(pl.multiple_of(LANES * h, LANES), LANES)
                for i in range(n):
                    tile(n * h + i)
                u, w = _factor128(diag[span, span])
                for i in range(LANES // GROUP):
                    at = pl.ds(pl.multiple_of(LANES * h + GROUP * i, GROUP), GROUP)
                    upper[GROUP * i : GROUP * i + GROUP, :] = u[i]
                    inv[at, span] = w[i]
                lower[span, span] = upper[...].T

                @pl.when(more & (h == 0))
                def _():
                    relay_one(now, w0)

            each(0, 2, half)

        a_block = jnp.where(count >= 8, 4, jnp.where(count >= 4, 2, 1))
        for n in (4, 2, 1):
            @pl.when(a_block == n)
            def _():
                chain(n)

        @pl.when(more)
        def _():
            forward_small(par)

        inv[LANES:, :LANES] = -_nn(inv[LANES:, LANES:], _nn(lower[LANES:, :LANES], inv[:LANES, :LANES]))
        inv[:LANES, LANES:] = jnp.zeros((LANES, LANES), F32)
        lower[:LANES, LANES:] = jnp.zeros((LANES, LANES), F32)
        for i in range(4):
            s0, s1 = _swap_middle(inv[TR * ORDER[i] : TR * ORDER[i] + TR, :LANES], inv[TR * ORDER[i] : TR * ORDER[i] + TR, LANES:])
            invp[par, TR * i : TR * i + TR, :LANES] = s0
            invp[par, TR * i : TR * i + TR, LANES:] = s1

        many = parts - 1 - w0
        over = jnp.maximum(count - 2 * a_block, 0)

        def share(j):
            return 2 * a_block + (over * j) // jnp.maximum(many, 1)

        def between(j):
            each(share(j), share(j + 1), tile)

            @pl.when(more)
            def _():
                relay_one(now, w0 + 1 + j)

        each(0, jnp.where(more, many, 0), between)
        each(jnp.where(more & (many > 0), count, 2 * a_block), count, tile)

        @pl.when(more)
        def _():
            finish_small(par)
            for i in range(4):
                a1[TR * i : TR * i + TR, :LANES] = pieces[par, 2 * i, :TR, :]
                a1[TR * i : TR * i + TR, LANES:] = pieces[par, 2 * i + 1, :TR, :]
            place_diag(par)
            x1 = _nt(a1[...], invp[par])
            diag[...] = diag[...] - _nt(x1, x1)

        def put(q):
            return pltpu.make_async_copy(xl.at[rows_of(q), pl.ds(own, TC)], out_hbm.at[rows_of(q), cols_of(k)], out_sem.at[q])

        def put_zero(q, at):
            return pltpu.make_async_copy(zeros, out_hbm.at[rows_of(q), cols_of(at)], out_sem.at[q])

        @pl.when(k > 0)
        def _():
            each(0, chunks, lambda q: put_zero(q, k - 1).wait())

        @pl.when(more)
        def _():
            def solve_left(q):
                xl[rows_of(q), :] = _nt(left[now, pl.ds(QS * q, QS)].reshape(QS * TR, SB), invp[par])

            each((k + 1) // QS, chunks, solve_left)
        @pl.when(more)
        def _():
            each(w0, jnp.minimum((k + 2) // WS + 1, parts), lambda w: relay_two(now, w))
            xrt[:, cols_of(pair, 2)] = _nt(invp[par], right[now, pl.ds(pair, 2)].reshape(4 * TR, SB))

        def clear_above(i):
            xl[pl.ds(pl.multiple_of(TR * i, TR), TR), :] = jnp.zeros((TR, SB), F32)

        each(QS * q0, k, clear_above)
        mine = pl.ds(pl.multiple_of(TR * r, TR), TR)
        s0, s1 = _swap_middle(lower[mine, :LANES], lower[mine, LANES:])
        at = pl.ds(pl.multiple_of(TR * k, TR), TR)
        xl[at, :LANES] = s0
        xl[at, LANES:] = s1
        each(0, q0, lambda q: put_zero(q, k).start())
        each(q0, chunks, lambda q: put(q).start())

        @pl.when(more)
        def _():
            cs = cols_of(pair, 2)

            def update(q):
                mat[rows_of(q), cs] = mat[rows_of(q), cs] - _nn(xl[rows_of(q), :], xrt[:, cs])

            each((k + 1) // QS, chunks, update)

        @pl.when(k > 0)
        def _():
            each(k // WS, parts, lambda w: sent(last, w))
        return carry

    lax.fori_loop(0, steps, step, 0)
    each(0, chunks, lambda q: pltpu.make_async_copy(zeros, out_hbm.at[rows_of(q), cols_of(steps - 1)], out_sem.at[q]).wait())


def solution(mesh):
    def local_factor(blocks):
        row_blocks, block_size, local_cols = blocks.shape
        rows = row_blocks * block_size
        steps = local_cols // TC
        chunks, parts = steps // QS, steps // WS
        dma = pltpu.SemaphoreType.DMA
        vm = lambda *s: pltpu.VMEM(s, F32)
        out = pl.pallas_call(
            lambda *refs: _kernel(steps, *refs),
            out_shape=jax.ShapeDtypeStruct((rows, local_cols), F32),
            in_specs=[pl.BlockSpec(memory_space=pl.ANY)],
            out_specs=pl.BlockSpec(memory_space=pl.ANY),
            scratch_shapes=[
                vm(rows, local_cols),
                vm(3, steps, TR, SB),
                vm(3, steps, 2, TR, SB),
                vm(rows, SB),
                vm(SB, local_cols),
                vm(2, 8, 2 * TR, TC),
                vm(SB, SB),
                vm(LANES, LANES),
                vm(SB, SB),
                vm(SB, SB),
                vm(2, SB, SB),
                vm(SB, SB),
                vm(QS * TR, TC),
                dma((chunks + 1,)),
                dma((chunks,)),
                dma((2, 4)),
                dma((2, 4)),
                dma((2, 3)),
                dma((2, 3)),
                dma((3, parts)),
                dma((3, parts)),
                dma((3, parts, 2)),
                dma((3, parts, 2)),
                dma((3, parts, 2)),
                dma((3, parts, 2)),
            ],
            compiler_params=pltpu.CompilerParams(has_side_effects=True, vmem_limit_bytes=67043328),
            name="cholesky",
        )(blocks.reshape(rows, local_cols))
        return out.reshape(row_blocks, block_size, local_cols)

    spec = P(("part", "row"), None, "col")
    return jax.shard_map(local_factor, mesh=mesh, in_specs=(spec,), out_specs=spec, check_vma=False)
```

```python
import jax
import jax.numpy as jnp
from jax import lax
from jax.experimental import pallas as pl
from jax.experimental.pallas import tpu as pltpu
from jax.sharding import PartitionSpec as P

F32 = jnp.float32
FULL = lax.Precision.HIGHEST
SB = 256
TR = 64
TC = 128
LANES = 128
GROUP = 8
CHUNK = 32
QS = 4
WS = 2
PER = QS // WS
TILE = 512
ORDER = (0, 2, 1, 3)


def _nn(a, b):
    return lax.dot_general(a, b, (((1,), (0,)), ((), ())), precision=FULL, preferred_element_type=F32)


def _nt(a, b):
    return lax.dot_general(a, b, (((1,), (1,)), ((), ())), precision=FULL, preferred_element_type=F32)


def _swap_middle(x0, x1):
    low = lax.broadcasted_iota(jnp.int32, x0.shape, 1) < LANES // 2
    half = LANES // 2
    return jnp.where(low, x0, pltpu.roll(x1, half, 1)), jnp.where(low, pltpu.roll(x0, half, 1), x1)


def _factor128(src):
    size = LANES
    lane = lax.broadcasted_iota(jnp.int32, (size, LANES), 1)
    rows = lax.broadcasted_iota(jnp.int32, (size, LANES), 0)
    left = src
    right = jnp.where(lane == rows, 1.0, 0.0).astype(F32)
    rid = lax.broadcasted_iota(jnp.int32, (GROUP, LANES), 0)
    lid = lax.broadcasted_iota(jnp.int32, (GROUP, LANES), 1)
    upper, inverse = [], []
    for g in range(size // GROUP):
        base = GROUP * g
        top_l, top_r = left[:GROUP], right[:GROUP]
        cols = [jnp.broadcast_to(top_l[:, base + j : base + j + 1], (GROUP, LANES)) for j in range(GROUP)]
        scale, row_l, row_r, mult = [], [], [], {}
        for j in range(GROUP):
            inv = lax.rsqrt(cols[j][j : j + 1])
            low = jnp.where(rid > j, cols[j] * inv, 0.0)
            u_l, u_r = top_l[j : j + 1] * inv, top_r[j : j + 1] * inv
            for k in range(j + 1, GROUP):
                mult[j, k] = cols[k][j : j + 1] * inv
                cols[k] = cols[k] - low * mult[j, k]
            top_l = jnp.where(rid == j, u_l, top_l - low * u_l)
            top_r = jnp.where(rid == j, u_r, top_r - low * u_r)
            scale.append(inv)
            row_l.append(u_l)
            row_r.append(u_r)
        upper.append(jnp.where(lid >= rid + base, top_l, 0.0))
        inverse.append(top_r)
        rest = size - base - GROUP
        if rest == 0:
            break
        next_l, next_r = [], []
        for start in range(0, rest, CHUNK):
            stop = min(start + CHUNK, rest)
            a, b = left[GROUP + start : GROUP + stop], right[GROUP + start : GROUP + stop]
            below = [jnp.broadcast_to(a[:, base + j : base + j + 1], (stop - start, LANES)) for j in range(GROUP)]
            for j in range(GROUP):
                low = below[j] * scale[j]
                for k in range(j + 1, GROUP):
                    below[k] = below[k] - low * mult[j, k]
                a = a - low * row_l[j]
                b = b - low * row_r[j]
            next_l.append(a)
            next_r.append(b)
        left = jnp.concatenate(next_l, 0) if len(next_l) > 1 else next_l[0]
        right = jnp.concatenate(next_r, 0) if len(next_r) > 1 else next_r[0]
    return upper, inverse


def _kernel(steps, a_hbm, out_hbm, mat, left, right, xl, yl, pieces, diag, upper, lower, inv, invp, a1, zeros,
            load_sem, out_sem, sg_send, sg_recv, fw_send, fw_recv, f1_send, f1_recv, f2_send, f2_recv, f3_send, f3_recv):
    r = lax.axis_index("row")
    c = lax.axis_index("col")
    x = r // 2
    p = r % 2
    me = r * 2 + c
    major = p == c
    chunks = steps // QS
    parts = steps // WS
    rows, cols = steps * TR, steps * TC
    tiles = rows // TILE
    own = pl.multiple_of(c * TC, TC)
    other = pl.multiple_of((1 - c) * TC, TC)
    xi = (r + 2) % 4
    y_peer = {"row": r, "col": 1 - c}
    x_peer = {"row": xi, "col": c}
    z_peer = {"row": xi, "col": 1 - c}
    d_peer = {"row": 2 * x + 1 - p, "col": c}
    peers = (d_peer, y_peer, x_peer, z_peer)

    def small(par, i):
        return pltpu.make_async_remote_copy(pieces.at[par, me], pieces.at[par, me], sg_send.at[par, i],
                                            sg_recv.at[par, i], device_id=peers[i])

    sources = (None, r * 2 + 1 - c, xi * 2 + c, xi * 2 + 1 - c)

    def forward(par, i):
        return pltpu.make_async_remote_copy(pieces.at[par, sources[i]], pieces.at[par, sources[i]], fw_send.at[par, i - 1],
                                            fw_recv.at[par, i - 1], device_id=d_peer)

    def start_small(par):
        for i in range(4):
            small(par, i).start()

    def forward_small(par):
        small(par, 0).wait_recv()
        for i in range(1, 4):
            small(par, i).wait_recv()
            forward(par, i).start()

    def finish_small(par):
        for i in range(1, 4):
            forward(par, i).wait_recv()
        for i in range(4):
            small(par, i).wait_send()
        for i in range(1, 4):
            forward(par, i).wait_send()

    def f1(par, w):
        ref = left.at[par, pl.ds(WS * w, WS), :, pl.ds(own, TC)]
        return pltpu.make_async_remote_copy(ref, ref, f1_send.at[par, w], f1_recv.at[par, w], device_id=y_peer)

    def f2(par, w, h, at):
        return pltpu.make_async_remote_copy(left.at[par, pl.ds(WS * w, WS), :, pl.ds(at, TC)],
                                            right.at[par, pl.ds(WS * w, WS), x, :, pl.ds(at, TC)],
                                            f2_send.at[par, w, h], f2_recv.at[par, w, h], device_id=x_peer)

    def f3a(par, w):
        return pltpu.make_async_remote_copy(left.at[par, pl.ds(WS * w, WS)], right.at[par, pl.ds(WS * w, WS), x],
                                            f3_send.at[par, w, 0], f3_recv.at[par, w, 0], device_id=d_peer)

    def f3b(par, w):
        ref = right.at[par, pl.ds(WS * w, WS), 1 - x]
        return pltpu.make_async_remote_copy(ref, ref, f3_send.at[par, w, 1], f3_recv.at[par, w, 1], device_id=d_peer)

    def relay_one(par, w):
        f1(par, w).wait_recv()

        @pl.when(major)
        def _():
            f2(par, w, 1, other).start()
            f3a(par, w).start()
            right[par, pl.ds(WS * w, WS), x] = left[par, pl.ds(WS * w, WS)]

    def pass_on(par, w):
        @pl.when(major)
        def _():
            f2(par, w, 0, own).wait_recv()
            f2(par, w, 1, other).wait_recv()
            f3b(par, w).start()

    def take(par, w):
        @pl.when(jnp.logical_not(major))
        def _():
            f3a(par, w).wait_recv()
            f3b(par, w).wait_recv()

    def relay_two(par, w):
        pass_on(par, w)
        take(par, w)

    def sent(par, w):
        f1(par, w).wait_send()

        @pl.when(major)
        def _():
            f2(par, w, 0, own).wait_send()
            f2(par, w, 1, other).wait_send()
            f3a(par, w).wait_send()

    def rows_of(q):
        return pl.ds(pl.multiple_of(QS * TR * q, QS * TR), QS * TR)

    def cols_of(k, n=1):
        return pl.ds(pl.multiple_of(TC * k, TC), n * TC)

    def each(lo, hi, body):
        def step(i, carry):
            body(i)
            return carry

        lax.fori_loop(lo, hi, step, 0)

    head = min(3 * TC, cols)

    def load_head():
        return pltpu.make_async_copy(a_hbm.at[:, pl.ds(0, head)], mat.at[:, pl.ds(0, head)], load_sem.at[chunks])

    def load_rest(q):
        wide = min((QS * TC) * (q + 2), cols) - head
        at = (pl.ds(QS * TR * q, QS * TR), pl.ds(head, wide))
        return pltpu.make_async_copy(a_hbm.at[at], mat.at[at], load_sem.at[q])

    load_head().start()
    barrier = pltpu.get_barrier_semaphore()
    for peer in peers:
        pl.semaphore_signal(barrier, inc=1, device_id=peer)
    zeros[...] = jnp.zeros_like(zeros)
    load_head().wait()
    for q in range(chunks):
        load_rest(q).start()
    pl.semaphore_wait(barrier, len(peers))

    def place_diag(par):
        for i in range(4):
            s0, s1 = _swap_middle(pieces[par, 2 * i, TR:, :], pieces[par, 2 * i + 1, TR:, :])
            diag[TR * i : TR * i + TR, :LANES] = s0
            diag[TR * i : TR * i + TR, LANES:] = s1

    def stage(k, w):
        slot = k % 3
        f1(slot, w).start()

        @pl.when(major)
        def _():
            f2(slot, w, 0, own).start()

    def stage_small(k):
        slot = k % 3
        nxt = pl.ds(pl.multiple_of(TR * (k + 1), TR), TR)
        pieces[slot, me, :TR, :] = mat[nxt, cols_of(k)]
        pieces[slot, me, TR:, :] = mat[nxt, cols_of(k + 1)]
        start_small(slot)

    pieces[2, me, :TR, :] = jnp.zeros((TR, TC), F32)
    pieces[2, me, TR:, :] = mat[:TR, :TC]
    start_small(2)

    def first(q):
        left[0, pl.ds(QS * q, QS), :, pl.ds(own, TC)] = mat[rows_of(q), :TC].reshape(QS, TR, TC)

    each(0, chunks, first)
    stage(0, 0)
    stage_small(0)
    each(1, parts, lambda w: stage(0, w))
    forward_small(2)
    finish_small(2)
    place_diag(2)

    def step(k, carry):
        now = k % 3
        last = (k + 2) % 3
        q0 = k // QS
        w0 = (k + 1) // WS
        more = k < steps - 1
        pair = jnp.minimum(k + 1, steps - 2)
        w1 = jnp.minimum((k + 2) // WS, parts - 1)
        ahead = w1 + 1

        u0 = (k + 2) // QS
        count = 0
        for t in range(tiles):
            count = count + jnp.maximum(2 * t + 2 - u0, 0)
        count = jnp.where(k > 0, count, 0)

        def tile(i):
            t, first, total = 0, 0, 0
            for s in range(tiles):
                total = total + jnp.maximum(2 * s + 2 - u0, 0)
                past = i >= total
                t = t + jnp.where(past, 1, 0)
                first = jnp.where(past, total, first)
            live = i < count
            t = jnp.where(live, t, 0)
            u = jnp.where(live, u0 + i - first, 2 * tiles - 1)
            rs = pl.ds(pl.multiple_of(TILE * t, TILE), TILE)
            cs = pl.ds(pl.multiple_of(TILE * u, TILE), TILE)
            mat[rs, cs] = mat[rs, cs] - _nt(yl[rs, :], right[last, pl.ds(QS * u, QS)].reshape(TILE, SB))

        @pl.when(k > 0)
        def _():
            each((k + 1) // WS + 1, parts, lambda w: relay_two(last, w))

            @pl.when(major)
            def _():
                each(k // WS, jnp.minimum((k + 1) // WS + 1, parts), lambda w: f3b(last, w).wait_send())

            right[last, pl.ds(jnp.minimum(k, steps - 2), 2)] = jnp.zeros((2, 2, TR, SB), F32)

        @pl.when(k == 1)
        def _():
            for q in range(chunks):
                load_rest(q).wait()

        def chain(n):
            def half(h):
                @pl.when(h == 1)
                def _():
                    w00 = inv[:LANES, :LANES]
                    l10 = _nt(diag[LANES:, :LANES], w00)
                    lower[LANES:, :LANES] = l10
                    diag[LANES:, LANES:] = diag[LANES:, LANES:] - _nt(l10, l10)

                span = pl.ds(pl.multiple_of(LANES * h, LANES), LANES)
                for i in range(n):
                    tile(n * h + i)
                u, w = _factor128(diag[span, span])
                for i in range(LANES // GROUP):
                    at = pl.ds(pl.multiple_of(LANES * h + GROUP * i, GROUP), GROUP)
                    upper[GROUP * i : GROUP * i + GROUP, :] = u[i]
                    inv[at, span] = w[i]
                lower[span, span] = upper[...].T

                @pl.when(more & (h == 0))
                def _():
                    forward_small(now)
                    each(w0, ahead, lambda w: relay_one(now, w))

            each(0, 2, half)

        a_block = jnp.where(count >= 8, 4, jnp.where(count >= 4, 2, 1))
        for n in (4, 2, 1):
            @pl.when(a_block == n)
            def _():
                chain(n)

        @pl.when(more)
        def _():
            each(w0, w1 + 1, lambda w: pass_on(now, w))

        inv[LANES:, :LANES] = -_nn(inv[LANES:, LANES:], _nn(lower[LANES:, :LANES], inv[:LANES, :LANES]))
        inv[:LANES, LANES:] = jnp.zeros((LANES, LANES), F32)
        lower[:LANES, LANES:] = jnp.zeros((LANES, LANES), F32)
        for i in range(4):
            s0, s1 = _swap_middle(inv[TR * ORDER[i] : TR * ORDER[i] + TR, :LANES], inv[TR * ORDER[i] : TR * ORDER[i] + TR, LANES:])
            invp[TR * i : TR * i + TR, :LANES] = s0
            invp[TR * i : TR * i + TR, LANES:] = s1

        def put(q):
            return pltpu.make_async_copy(xl.at[rows_of(q), pl.ds(own, TC)], out_hbm.at[rows_of(q), cols_of(k)], out_sem.at[q])

        def put_zero(q, at):
            return pltpu.make_async_copy(zeros, out_hbm.at[rows_of(q), cols_of(at)], out_sem.at[q])

        many = parts - ahead
        over = jnp.maximum(count - 2 * a_block, 0)

        def share(j):
            return 2 * a_block + (over * j) // jnp.maximum(many, 1)

        def between(j):
            each(share(j), share(j + 1), tile)
            relay_one(now, ahead + j)

        each(0, jnp.where(more, many, 0), between)
        each(jnp.where(more & (many > 0), count, 2 * a_block), count, tile)

        @pl.when(k > 0)
        def _():
            each(k // WS, parts, lambda w: sent(last, w))

            @pl.when(major)
            def _():
                each((k + 1) // WS + 1, parts, lambda w: f3b(last, w).wait_send())

            each(0, chunks, lambda q: put_zero(q, k - 1).wait())

        def chunk_of(q):
            return left[now, pl.ds(QS * q, QS)].reshape(QS * TR, SB)

        q1 = (k + 1) // QS
        q2 = jnp.minimum(q1 + 1, chunks - 1)

        @pl.when(more)
        def _():
            each(w0, w1 + 1, lambda w: take(now, w))
            finish_small(now)
            for i in range(4):
                a1[TR * i : TR * i + TR, :LANES] = pieces[now, 2 * i, :TR, :]
                a1[TR * i : TR * i + TR, LANES:] = pieces[now, 2 * i + 1, :TR, :]
            place_diag(now)
            x1 = _nt(a1[...], invp[...])
            xa = _nt(chunk_of(q1), invp[...])
            xb = _nt(chunk_of(q2), invp[...])
            diag[...] = diag[...] - _nt(x1, x1)
            yl[rows_of(q1), :] = _nn(xa, invp[...])
            xl[rows_of(q1), :] = xa
            xl[rows_of(q2), :] = xb

        @pl.when(more)
        def _():
            cs = cols_of(pair, 2)
            slot = (k + 1) % 3

            def advance(q):
                qa, qb = jnp.minimum(q + 1, chunks - 1), jnp.minimum(q + 2, chunks - 1)
                xb = _nt(chunk_of(qb), invp[...])
                ya = _nn(xl[rows_of(qa), :], invp[...])
                new = mat[rows_of(q), cs] - _nt(yl[rows_of(q), :], right[now, pl.ds(pair, 2)].reshape(4 * TR, SB))
                mat[rows_of(q), cs] = new
                left[slot, pl.ds(QS * q, QS), :, pl.ds(own, TC)] = new[:, :TC].reshape(QS, TR, TC)
                yl[rows_of(qa), :] = ya
                xl[rows_of(qb), :] = xb

                @pl.when(k < steps - 2)
                def _():
                    for i in range(PER):
                        @pl.when(PER * q + i >= (k + 2) // WS)
                        def _():
                            stage(k + 1, PER * q + i)

                    @pl.when(q == (k + 2) // QS)
                    def _():
                        stage_small(k + 1)

            each(q1, chunks, advance)

        def clear_above(i):
            xl[pl.ds(pl.multiple_of(TR * i, TR), TR), :] = jnp.zeros((TR, SB), F32)

        each(QS * q0, k, clear_above)
        mine = pl.ds(pl.multiple_of(TR * r, TR), TR)
        s0, s1 = _swap_middle(lower[mine, :LANES], lower[mine, LANES:])
        at = pl.ds(pl.multiple_of(TR * k, TR), TR)
        xl[at, :LANES] = s0
        xl[at, LANES:] = s1
        each(0, q0, lambda q: put_zero(q, k).start())
        each(q0, chunks, lambda q: put(q).start())

        return carry

    lax.fori_loop(0, steps, step, 0)
    each(0, chunks, lambda q: pltpu.make_async_copy(zeros, out_hbm.at[rows_of(q), cols_of(steps - 1)], out_sem.at[q]).wait())


def solution(mesh):
    def local_factor(blocks):
        row_blocks, block_size, local_cols = blocks.shape
        rows = row_blocks * block_size
        steps = local_cols // TC
        chunks, parts = steps // QS, steps // WS
        dma = pltpu.SemaphoreType.DMA
        vm = lambda *s: pltpu.VMEM(s, F32)
        out = pl.pallas_call(
            lambda *refs: _kernel(steps, *refs),
            out_shape=jax.ShapeDtypeStruct((rows, local_cols), F32),
            in_specs=[pl.BlockSpec(memory_space=pl.ANY)],
            out_specs=pl.BlockSpec(memory_space=pl.ANY),
            scratch_shapes=[
                vm(rows, local_cols),
                vm(3, steps, TR, SB),
                vm(3, steps, 2, TR, SB),
                vm(rows, SB),
                vm(rows, SB),
                vm(3, 8, 2 * TR, TC),
                vm(SB, SB),
                vm(LANES, LANES),
                vm(SB, SB),
                vm(SB, SB),
                vm(SB, SB),
                vm(SB, SB),
                vm(QS * TR, TC),
                dma((chunks + 1,)),
                dma((chunks,)),
                dma((3, 4)),
                dma((3, 4)),
                dma((3, 3)),
                dma((3, 3)),
                dma((3, parts)),
                dma((3, parts)),
                dma((3, parts, 2)),
                dma((3, parts, 2)),
                dma((3, parts, 2)),
                dma((3, parts, 2)),
            ],
            compiler_params=pltpu.CompilerParams(collective_id=0, has_side_effects=True, vmem_limit_bytes=67043328),
            name="cholesky",
        )(blocks.reshape(rows, local_cols))
        return out.reshape(row_blocks, block_size, local_cols)

    spec = P(("part", "row"), None, "col")
    return jax.shard_map(local_factor, mesh=mesh, in_specs=(spec,), out_specs=spec, check_vma=False)
```

```python
import jax
import jax.numpy as jnp
from jax import lax
from jax.experimental import pallas as pl
from jax.experimental.pallas import tpu as pltpu
from jax.sharding import PartitionSpec as P

F32 = jnp.float32
FULL = lax.Precision.HIGHEST
SB = 256
TR = 64
TC = 128
LANES = 128
CHUNK = 64
QS = 4
WS = 2
PER = QS // WS
LOT = 6
NARROW = 4
TILE = 512
LAST = 2
ORDER = (0, 2, 1, 3)


def _nn(a, b):
    return lax.dot_general(a, b, (((1,), (0,)), ((), ())), precision=FULL, preferred_element_type=F32)


def _nt(a, b):
    return lax.dot_general(a, b, (((1,), (1,)), ((), ())), precision=FULL, preferred_element_type=F32)


def _swap_middle(x0, x1):
    low = lax.broadcasted_iota(jnp.int32, x0.shape, 1) < LANES // 2
    half = LANES // 2
    return jnp.where(low, x0, pltpu.roll(x1, half, 1)), jnp.where(low, pltpu.roll(x0, half, 1), x1)


def _eliminate(left, right, first, count, group):
    rid = lax.broadcasted_iota(jnp.int32, (group, LANES), 0)
    lid = lax.broadcasted_iota(jnp.int32, (group, LANES), 1)
    upper, inverse = [], []
    for g in range(count // group):
        base = first + group * g
        top_l, top_r = left[:group], right[:group]
        cols = [jnp.broadcast_to(top_l[:, base + j : base + j + 1], (group, LANES)) for j in range(group)]
        scale, row_l, row_r, mult = [], [], [], {}
        for j in range(group):
            inv = lax.rsqrt(cols[j][j : j + 1])
            low = jnp.where(rid > j, cols[j] * inv, 0.0)
            u_l, u_r = top_l[j : j + 1] * inv, top_r[j : j + 1] * inv
            for k in range(j + 1, group):
                mult[j, k] = cols[k][j : j + 1] * inv
                cols[k] = cols[k] - low * mult[j, k]
            top_l = jnp.where(rid == j, u_l, top_l - low * u_l)
            top_r = jnp.where(rid == j, u_r, top_r - low * u_r)
            scale.append(inv)
            row_l.append(u_l)
            row_r.append(u_r)
        upper.append(jnp.where(lid >= rid + base, top_l, 0.0))
        inverse.append(top_r)
        rest = count - group * (g + 1)
        if rest == 0:
            break
        next_l, next_r = [], []
        for start in range(0, rest, CHUNK):
            stop = min(start + CHUNK, rest)
            a, b = left[group + start : group + stop], right[group + start : group + stop]
            below = [jnp.broadcast_to(a[:, base + j : base + j + 1], (stop - start, LANES)) for j in range(group)]
            for j in range(group):
                low = below[j] * scale[j]
                for k in range(j + 1, group):
                    below[k] = below[k] - low * mult[j, k]
                a = a - low * row_l[j]
                b = b - low * row_r[j]
            next_l.append(a)
            next_r.append(b)
        left = jnp.concatenate(next_l, 0) if len(next_l) > 1 else next_l[0]
        right = jnp.concatenate(next_r, 0) if len(next_r) > 1 else next_r[0]
    return upper, inverse


def _factor128(src, group, split):
    lane = lax.broadcasted_iota(jnp.int32, (LANES, LANES), 1)
    rows = lax.broadcasted_iota(jnp.int32, (LANES, LANES), 0)
    left, right = src, jnp.where(lane == rows, 1.0, 0.0).astype(F32)
    upper, inverse = [], []
    for first in range(0, LANES, split):
        u, w = _eliminate(left[:split], right[:split], first, split, group)
        upper += u
        inverse += w
        if first + split < LANES:
            u, w = jnp.concatenate(u, 0), jnp.concatenate(w, 0)
            t = u.T[first + split :]
            left, right = left[split:] - _nn(t, u), right[split:] - _nn(t, w)
    return upper, inverse


def _half(diag, upper, lower, inv, h, group, split):
    span = pl.ds(pl.multiple_of(LANES * h, LANES), LANES)
    u, w = _factor128(diag[span, span], group, split)
    for i in range(LANES // group):
        at = pl.ds(pl.multiple_of(LANES * h + group * i, group), group)
        upper[group * i : group * i + group, :] = u[i]
        inv[at, span] = w[i]
    lower[span, span] = upper[...].T


def _middle(diag, lower, inv):
    l10 = _nt(diag[LANES:, :LANES], inv[:LANES, :LANES])
    lower[LANES:, :LANES] = l10
    diag[LANES:, LANES:] = diag[LANES:, LANES:] - _nt(l10, l10)


def _inverse(lower, inv, invp):
    inv[LANES:, :LANES] = -_nn(inv[LANES:, LANES:], _nn(lower[LANES:, :LANES], inv[:LANES, :LANES]))
    inv[:LANES, LANES:] = jnp.zeros((LANES, LANES), F32)
    lower[:LANES, LANES:] = jnp.zeros((LANES, LANES), F32)
    for i in range(4):
        at = slice(TR * ORDER[i], TR * ORDER[i] + TR)
        s0, s1 = _swap_middle(inv[at, :LANES], inv[at, LANES:])
        invp[TR * i : TR * i + TR, :LANES] = s0
        invp[TR * i : TR * i + TR, LANES:] = s1


def _own_rows(lower, r):
    mine = pl.ds(pl.multiple_of(TR * r, TR), TR)
    return _swap_middle(lower[mine, :LANES], lower[mine, LANES:])


def _each(lo, hi, body):
    def step(i, carry):
        body(i)
        return carry

    lax.fori_loop(lo, hi, step, 0)


def _rows_of(q):
    return pl.ds(pl.multiple_of(QS * TR * q, QS * TR), QS * TR)


def _cols_of(k, n=1):
    return pl.ds(pl.multiple_of(TC * k, TC), n * TC)


def _kernel(steps, a_hbm, out_hbm, rest_hbm, mat, left, right, xl, yl, pieces, diag, upper, lower, inv, invp, a1, pair,
            load_sem, out_sem, sg_send, sg_recv, fw_send, fw_recv, f1_send, f1_recv, f2_send, f2_recv, f3_send, f3_recv):
    r = lax.axis_index("row")
    c = lax.axis_index("col")
    x = r // 2
    p = r % 2
    me = r * 2 + c
    major = p == c
    minor = p != c
    chunks = steps // QS
    parts = steps // WS
    end = steps - LAST
    late = steps - 8
    rows, cols = steps * TR, steps * TC
    tiles = rows // TILE
    wide_u = max(u for u in range(2 * tiles) if sum(tiles - s // 2 for s in range(u, 2 * tiles)) > 4)
    own = pl.multiple_of(c * TC, TC)
    other = pl.multiple_of((1 - c) * TC, TC)
    xi = (r + 2) % 4
    y_peer = {"row": r, "col": 1 - c}
    x_peer = {"row": xi, "col": c}
    z_peer = {"row": xi, "col": 1 - c}
    d_peer = {"row": 2 * x + 1 - p, "col": c}
    peers = (d_peer, y_peer, x_peer, z_peer)
    each, rows_of, cols_of = _each, _rows_of, _cols_of

    def small(slot, i, n):
        ref = pieces.at[slot, me, pl.ds(0, n * TR)]
        return pltpu.make_async_remote_copy(ref, ref, sg_send.at[slot, i], sg_recv.at[slot, i], device_id=peers[i])

    sources = (None, r * 2 + 1 - c, xi * 2 + c, xi * 2 + 1 - c)

    def forward(slot, i, n):
        ref = pieces.at[slot, sources[i], pl.ds(0, n * TR)]
        return pltpu.make_async_remote_copy(ref, ref, fw_send.at[slot, i - 1], fw_recv.at[slot, i - 1], device_id=d_peer)

    def by_size(k, body):
        for n, chosen in ((2, k < late), (3, k >= late)):
            @pl.when(chosen)
            def _():
                body(n)

    def start_small(k):
        def body(n):
            for i in range(4):
                small((k + 3) % 3, i, n).start()

        by_size(k, body)

    def forward_small(k):
        def body(n):
            small((k + 3) % 3, 0, n).wait_recv()
            for i in range(1, 4):
                small((k + 3) % 3, i, n).wait_recv()
                forward((k + 3) % 3, i, n).start()

        by_size(k, body)

    def finish_small(k):
        def body(n):
            for i in range(1, 4):
                forward((k + 3) % 3, i, n).wait_recv()
            for i in range(4):
                small((k + 3) % 3, i, n).wait_send()
            for i in range(1, 4):
                forward((k + 3) % 3, i, n).wait_send()

        by_size(k, body)

    def f1(slot, w):
        ref = left.at[slot, pl.ds(WS * w, WS), :, pl.ds(own, TC)]
        return pltpu.make_async_remote_copy(ref, ref, f1_send.at[slot, w], f1_recv.at[slot, w], device_id=y_peer)

    def f2(slot, w, h, at):
        return pltpu.make_async_remote_copy(left.at[slot, pl.ds(WS * w, WS), :, pl.ds(at, TC)],
                                            right.at[slot, pl.ds(WS * w, WS), x, :, pl.ds(at, TC)],
                                            f2_send.at[slot, w, h], f2_recv.at[slot, w, h], device_id=x_peer)

    def f3a(slot, w):
        return pltpu.make_async_remote_copy(left.at[slot, pl.ds(WS * w, WS)], right.at[slot, pl.ds(WS * w, WS), x],
                                            f3_send.at[slot, w, 0], f3_recv.at[slot, w, 0], device_id=d_peer)

    def f3b(slot, w):
        ref = right.at[slot, pl.ds(WS * w, WS), 1 - x]
        return pltpu.make_async_remote_copy(ref, ref, f3_send.at[slot, w, 1], f3_recv.at[slot, w, 1], device_id=d_peer)

    def relay(k, w):
        slot = k % 3
        f1(slot, w).wait_recv()

        @pl.when(major & (k < end - 1))
        def _():
            f2(slot, w, 1, other).start()
            f3a(slot, w).start()
            right[slot, pl.ds(WS * w, WS), x] = left[slot, pl.ds(WS * w, WS)]

    def arrived(slot, w):
        f2(slot, w, 0, own).wait_recv()
        f2(slot, w, 1, other).wait_recv()

    def take(slot, w):
        f3a(slot, w).wait_recv()
        f3b(slot, w).wait_recv()

    def sent(slot, w):
        f1(slot, w).wait_send()

        @pl.when(major)
        def _():
            f2(slot, w, 0, own).wait_send()
            f2(slot, w, 1, other).wait_send()
            f3a(slot, w).wait_send()

    head = min(3 * TC, cols)

    def load_first():
        return pltpu.make_async_copy(a_hbm.at[:TR, :TC], pieces.at[2, me, TR : 2 * TR], load_sem.at[chunks + 1])

    def load_head():
        return pltpu.make_async_copy(a_hbm.at[:, pl.ds(0, head)], mat.at[:, pl.ds(0, head)], load_sem.at[chunks])

    def load_rest(q):
        wide = min((QS * TC) * (q + 2), cols) - head
        at = (pl.ds(QS * TR * q, QS * TR), pl.ds(head, wide))
        return pltpu.make_async_copy(a_hbm.at[at], mat.at[at], load_sem.at[q])

    load_first().start()
    load_head().start()
    barrier = pltpu.get_barrier_semaphore()
    for peer in peers:
        pl.semaphore_signal(barrier, inc=1, device_id=peer)
    pieces[2, me, :TR] = jnp.zeros((TR, TC), F32)
    pieces[2, me, 2 * TR :] = jnp.zeros((TR, TC), F32)
    load_first().wait()
    pl.semaphore_wait(barrier, len(peers))
    start_small(-1)
    load_head().wait()
    for q in range(chunks):
        load_rest(q).start()

    def place_diag(slot):
        for i in range(4):
            s0, s1 = _swap_middle(pieces[slot, 2 * i, TR : 2 * TR, :], pieces[slot, 2 * i + 1, TR : 2 * TR, :])
            diag[TR * i : TR * i + TR, :LANES] = s0
            diag[TR * i : TR * i + TR, LANES:] = s1

    def place_next(slot):
        for i in range(4):
            a1[TR * i : TR * i + TR, :LANES] = pieces[slot, 2 * i, :TR, :]
            a1[TR * i : TR * i + TR, LANES:] = pieces[slot, 2 * i + 1, :TR, :]

    def stage(k, w):
        f1(k % 3, w).start()

    def stage_x(k, lot):
        @pl.when(major & (k < end - 1))
        def _():
            w0 = (k + 1) // WS
            cut = jnp.minimum(w0 + LOT, parts)
            each(jnp.where(lot == 0, w0, cut), jnp.where(lot == 0, cut, parts), lambda w: f2(k % 3, w, 0, own).start())

    def stage_small(k):
        slot = k % 3
        one = pl.ds(pl.multiple_of(TR * (k + 1), TR), TR)
        two = pl.ds(pl.multiple_of(TR * jnp.minimum(k + 2, steps - 1), TR), TR)
        pieces[slot, me, :TR, :] = mat[one, cols_of(k)]
        pieces[slot, me, TR : 2 * TR, :] = mat[one, cols_of(k + 1)]
        pieces[slot, me, 2 * TR :, :] = mat[two, cols_of(k)]
        start_small(k)

    def first(q):
        left[0, pl.ds(QS * q, QS), :, pl.ds(own, TC)] = mat[rows_of(q), :TC].reshape(QS, TR, TC)

    each(0, chunks, first)
    stage(0, 0)
    stage(0, 1)
    stage_small(0)
    each(2, parts, lambda w: stage(0, w))
    stage_x(0, 0)
    forward_small(-1)
    finish_small(-1)
    place_diag(2)

    def step(k, carry):
        now = k % 3
        last = (k + 2) % 3
        q0 = k // QS
        w0 = (k + 1) // WS
        w1 = jnp.minimum((k + 2) // WS, parts - 1)

        u0 = (k + 2) // QS
        count = 0
        for u in range(2 * tiles):
            count = count + jnp.where(u >= u0, tiles - u // 2, 0)
        count = jnp.where(k > 0, count, 0)

        inner = 0
        for u in range(2 * tiles):
            inner = inner + jnp.where((u >= u0) & (u < u0 + 3), tiles - u // 2, 0)
        inner = jnp.minimum(inner, 8)

        def tile(i, among=count):
            u, past_of, total = 0, 0, 0
            for s in range(2 * tiles):
                total = total + jnp.where(s >= u0, tiles - s // 2, 0)
                past = i >= total
                u = u + jnp.where(past, 1, 0)
                past_of = jnp.where(past, total, past_of)
            live = i < among
            t = jnp.where(live, u // 2 + i - past_of, 0)
            seen = jnp.where(live, u, u0)
            u = jnp.where(live, u, 2 * tiles - 1)
            rs = pl.ds(pl.multiple_of(TILE * t, TILE), TILE)
            cs = pl.ds(pl.multiple_of(TILE * u, TILE), TILE)
            mat[rs, cs] = mat[rs, cs] - _nt(yl[rs, :], right[last, pl.ds(QS * seen, QS)].reshape(TILE, SB))

        lo = k // WS
        mid = jnp.minimum((k + 1) // WS + 1, parts)
        s1 = jnp.clip(PER * (u0 + 2), mid, parts)
        s2 = jnp.clip(PER * (u0 + 3), mid, parts)

        def pass_on(slot, a, b):
            def body(w):
                arrived(slot, w)
                f3b(slot, w).start()

            each(a, b, body)

        def finish_exchange(passed, taken):
            @pl.when((k > 0) & major)
            def _():
                pass_on(last, *passed)

            @pl.when((k > 0) & minor)
            def _():
                each(*taken, lambda w: take(last, w))

        def finish_pair(side):
            zero = jnp.zeros((2, 2, TR, SB), F32)

            @pl.when((k > 0) & side)
            def _():
                @pl.when((k <= late) & major)
                def _():
                    each(lo, mid, lambda w: f3b(last, w).wait_send())

                @pl.when((k > late) & major)
                def _():
                    each(lo, mid, lambda w: arrived(last, w))

                @pl.when((k > late) & minor)
                def _():
                    each(lo, mid, lambda w: take(last, w))

                right[last, pl.ds(k, 2)] = zero

                @pl.when((k > late) & major)
                def _():
                    each(lo, mid, lambda w: f3b(last, w).start())

        def relay_pair():
            @pl.when(k < late)
            def _():
                each(w0, w1 + 1, lambda w: relay(k, w))

            stage_x(k, 1)

        wide = (k > 0) & (u0 <= wide_u)

        @pl.when(wide)
        def _():
            finish_pair(True)
            finish_exchange((s1, s2), (mid, s1))

            @pl.when(k == 1)
            def _():
                for q in range(chunks):
                    load_rest(q).wait()

            def half(h):
                @pl.when(h == 1)
                def _():
                    _middle(diag, lower, inv)
                    finish_exchange((s2, parts), (s1, s2))

                for i in range(4):
                    tile(4 * h + i, inner)
                _half(diag, upper, lower, inv, h, 8, LANES)

                @pl.when(h == 0)
                def _():
                    relay_pair()

            each(0, 2, half)

        @pl.when(jnp.logical_not(wide))
        def _():
            finish_pair(major)
            finish_exchange((mid, parts), (mid, mid))
            _half(diag, upper, lower, inv, 0, 16, LANES // 2)
            relay_pair()
            finish_pair(minor)
            finish_exchange((mid, mid), (mid, parts))
            _middle(diag, lower, inv)

        @pl.when(jnp.logical_not(wide))
        def _():
            for i in range(NARROW):
                tile(i)
            _half(diag, upper, lower, inv, 1, 8, LANES)

        forward_small(k)

        @pl.when((k < late) & major)
        def _():
            def body(w):
                arrived(now, w)
                f3b(now, w).start()

            each(w0, w1 + 1, body)

        _inverse(lower, inv, invp)

        @pl.when(wide)
        def _():
            finish_exchange((mid, mid), (s2, parts))

        def put(q, at):
            return pltpu.make_async_copy(xl.at[rows_of(q), pl.ds(own, TC)], out_hbm.at[rows_of(q), cols_of(at)], out_sem.at[q])

        q1 = (k + 1) // QS
        q2 = jnp.minimum(q1 + 1, chunks - 1)
        inner = jnp.where(wide, inner, jnp.minimum(count, NARROW))
        over = count - inner
        upto = jnp.minimum(jnp.maximum(w0 + 7 + (7 * over) // 10, PER * (q2 + 1)), parts)
        since = jnp.where(k < late, w1 + 1, w0)
        many = jnp.maximum(upto - since, 1)

        def share(j):
            return inner + (over * j) // many

        def between(j):
            each(share(j), share(j + 1), tile)

            @pl.when(since + j < upto)
            def _():
                relay(k, since + j)

        each(0, many, between)

        @pl.when(k > 0)
        def _():
            each(k // WS, parts, lambda w: sent(last, w))

            @pl.when(major)
            def _():
                each(jnp.where(k <= late, mid, lo), parts, lambda w: f3b(last, w).wait_send())

            each((k - 1) // QS, chunks, lambda q: put(q, k - 1).wait())

        def chunk_of(q):
            return left[now, pl.ds(QS * q, QS)].reshape(QS * TR, SB)

        def pair_of_pieces():
            for s in range(2):
                for h in range(2):
                    own_class = pieces.at[now, 2 * (c + 2 * s) + h]
                    pair[TR * s : TR * s + TR, TC * h : TC * h + TC] = own_class[:TR, :]
                    pair[TR * (2 + s) : TR * (2 + s) + TR, TC * h : TC * h + TC] = own_class[2 * TR :, :]

        finish_small(k)
        place_next(now)
        place_diag(now)

        @pl.when(k < late)
        def _():
            @pl.when(minor)
            def _():
                each(w0, w1 + 1, lambda w: take(now, w))

            pair[...] = right[now, pl.ds(k + 1, 2)].reshape(4 * TR, SB)

        @pl.when(k >= late)
        def _():
            pair_of_pieces()

        x1 = _nt(a1[...], invp[...])
        xa = _nt(chunk_of(q1), invp[...])
        xb = _nt(chunk_of(q2), invp[...])
        diag[...] = diag[...] - _nt(x1, x1)
        yl[rows_of(q1), :] = _nn(xa, invp[...])
        xl[rows_of(q1), :] = xa
        xl[rows_of(q2), :] = xb

        cs = cols_of(k + 1, 2)
        slot = (k + 1) % 3

        def advance(q):
            qa, qb = jnp.minimum(q + 1, chunks - 1), jnp.minimum(q + 2, chunks - 1)
            each(jnp.maximum(upto, PER * (q + 2)), jnp.minimum(PER * (q + 3), parts), lambda w: relay(k, w))
            xb = _nt(chunk_of(qb), invp[...])
            ya = _nn(xl[rows_of(qa), :], invp[...])
            new = mat[rows_of(q), cs] - _nt(yl[rows_of(q), :], pair[...])
            mat[rows_of(q), cs] = new
            left[slot, pl.ds(QS * q, QS), :, pl.ds(own, TC)] = new[:, :TC].reshape(QS, TR, TC)
            yl[rows_of(qa), :] = ya
            xl[rows_of(qb), :] = xb

            for i in range(PER):
                @pl.when((k < end - 1) & (PER * q + i >= (k + 2) // WS))
                def _():
                    stage(k + 1, PER * q + i)

            @pl.when(q == jnp.minimum(k + 3, steps - 1) // QS)
            def _():
                stage_small(k + 1)

        each(q1, chunks, advance)
        stage_x(k + 1, 0)

        def clear_above(i):
            xl[pl.ds(pl.multiple_of(TR * i, TR), TR), :] = jnp.zeros((TR, SB), F32)

        each(QS * q0, k, clear_above)
        at = pl.ds(pl.multiple_of(TR * k, TR), TR)
        xl[at, :LANES], xl[at, LANES:] = _own_rows(lower, r)
        each(q0, chunks, lambda q: put(q, k).start())

        u1 = (k + 3) // QS
        next_mid = jnp.minimum((k + 2) // WS + 1, parts)

        @pl.when(major & (u1 <= wide_u))
        def _():
            pass_on(now, next_mid, jnp.clip(PER * (u1 + 2), next_mid, parts))
        return carry

    lax.fori_loop(0, end, step, 0)

    def leave(src, i):
        return pltpu.make_async_copy(src, rest_hbm.at[i], load_sem.at[i])

    slot = end % 3
    leave(diag, 0).start()
    forward_small(end)
    finish_small(end)
    place_next(slot)
    leave(a1, 1).start()
    for i in range(4):
        s0, s1 = _swap_middle(pieces[slot, 2 * i, TR : 2 * TR, :], pieces[slot, 2 * i + 1, TR : 2 * TR, :])
        pair[TR * i : TR * i + TR, :LANES] = s0
        pair[TR * i : TR * i + TR, LANES:] = s1
    leave(pair, 2).start()
    for i, src in enumerate((diag, a1, pair)):
        leave(src, i).wait()
    each((end - 1 + 1) // WS, parts, lambda w: f1((end - 1) % 3, w).wait_send())

    def drain(q):
        pltpu.make_async_copy(xl.at[rows_of(q), pl.ds(own, TC)], out_hbm.at[rows_of(q), cols_of(end - 1)], out_sem.at[q]).wait()

    each((end - 1) // QS, chunks, drain)


def _finish(steps, part_hbm, rest, out_hbm, buf, zeros, diag, upper, lower, inv, invp, in_sem, out_sem, zero_sem):
    r = lax.axis_index("row")
    c = lax.axis_index("col")
    chunks = steps // QS
    rows, cols = steps * TR, steps * TC
    kept = cols - LAST * TC
    own = pl.multiple_of(c * TC, TC)

    def block(q):
        return (pl.ds(QS * TR * q, QS * TR), pl.ds(0, min(QS * TC * (q + 1), kept)))

    def load(q):
        return pltpu.make_async_copy(part_hbm.at[block(q)], buf.at[block(q)], in_sem.at[q])

    def store(q):
        return pltpu.make_async_copy(buf.at[block(q)], out_hbm.at[block(q)], out_sem.at[q])

    def blank(q):
        wide = cols - QS * TC * (q + 1)
        return pltpu.make_async_copy(zeros.at[:, pl.ds(0, wide)],
                                     out_hbm.at[pl.ds(QS * TR * q, QS * TR), pl.ds(QS * TC * (q + 1), wide)], zero_sem.at[q])

    tail = (pl.ds(rows - QS * TR, QS * TR), pl.ds(kept, LAST * TC))
    final = pltpu.make_async_copy(buf.at[tail], out_hbm.at[tail], zero_sem.at[chunks - 1])

    for q in range(chunks):
        load(q).start()
    zeros[...] = jnp.zeros_like(zeros)
    buf[tail] = jnp.zeros((QS * TR, LAST * TC), F32)

    def own_half(s0, s1):
        return jnp.where(c == 0, s0, s1)

    diag[...] = rest[0]
    for k in range(LAST):
        last_rows = slice(rows - (LAST - k) * TR, rows - (LAST - k - 1) * TR)
        at = slice(kept + k * TC, kept + k * TC + TC)
        _half(diag, upper, lower, inv, 0, 16, LANES // 2)
        _middle(diag, lower, inv)
        _half(diag, upper, lower, inv, 1, 16, LANES // 2)
        if k == 0:
            for q in range(chunks):
                load(q).wait()
                store(q).start()
            for q in range(chunks - 1):
                blank(q).start()
        if k < LAST - 1:
            _inverse(lower, inv, invp)
            x1 = _nt(rest[1], invp[...])
            diag[...] = rest[2] - _nt(x1, x1)
            upper_x = inv
            upper_x[...] = x1
            mine = pl.ds(pl.multiple_of(TR * r, TR), TR)
            buf[rows - TR :, at] = upper_x[mine, pl.ds(own, TC)]
        else:
            lower[:LANES, LANES:] = jnp.zeros((LANES, LANES), F32)
        buf[last_rows, at] = own_half(*_own_rows(lower, r))
    final.start()
    for q in range(chunks):
        store(q).wait()
    for q in range(chunks - 1):
        blank(q).wait()
    final.wait()


def solution(mesh):
    def local_factor(blocks):
        row_blocks, block_size, local_cols = blocks.shape
        rows = row_blocks * block_size
        steps = local_cols // TC
        chunks, parts = steps // QS, steps // WS
        dma = pltpu.SemaphoreType.DMA
        vm = lambda *s: pltpu.VMEM(s, F32)
        anywhere = pl.BlockSpec(memory_space=pl.ANY)
        shape = jax.ShapeDtypeStruct((rows, local_cols), F32)
        part, rest = pl.pallas_call(
            lambda *refs: _kernel(steps, *refs),
            out_shape=(shape, jax.ShapeDtypeStruct((3, SB, SB), F32)),
            in_specs=[anywhere],
            out_specs=(anywhere, anywhere),
            scratch_shapes=[
                vm(rows, local_cols),
                vm(3, steps, TR, SB),
                vm(3, steps, 2, TR, SB),
                vm(rows, SB),
                vm(rows, SB),
                vm(3, 8, 3 * TR, TC),
                vm(SB, SB),
                vm(LANES, LANES),
                vm(SB, SB),
                vm(SB, SB),
                vm(SB, SB),
                vm(SB, SB),
                vm(SB, SB),
                dma((chunks + 2,)),
                dma((chunks,)),
                dma((3, 4)),
                dma((3, 4)),
                dma((3, 3)),
                dma((3, 3)),
                dma((3, parts)),
                dma((3, parts)),
                dma((3, parts, 2)),
                dma((3, parts, 2)),
                dma((3, parts, 2)),
                dma((3, parts, 2)),
            ],
            compiler_params=pltpu.CompilerParams(collective_id=0, has_side_effects=True, vmem_limit_bytes=67043328),
            name="factor",
        )(blocks.reshape(rows, local_cols))
        out = pl.pallas_call(
            lambda *refs: _finish(steps, *refs),
            out_shape=shape,
            in_specs=[anywhere, pl.BlockSpec(memory_space=pltpu.VMEM)],
            out_specs=anywhere,
            scratch_shapes=[
                vm(rows, local_cols),
                vm(QS * TR, local_cols - QS * TC),
                vm(SB, SB),
                vm(LANES, LANES),
                vm(SB, SB),
                vm(SB, SB),
                vm(SB, SB),
                dma((chunks,)),
                dma((chunks,)),
                dma((chunks,)),
            ],
            compiler_params=pltpu.CompilerParams(vmem_limit_bytes=60 * 2**20),
            name="finish",
        )(part, rest)
        return out.reshape(row_blocks, block_size, local_cols)

    spec = P(("part", "row"), None, "col")
    return jax.shard_map(local_factor, mesh=mesh, in_specs=(spec,), out_specs=spec, check_vma=False)
```

```python
import jax
import jax.numpy as jnp
from jax import lax
from jax.experimental import pallas as pl
from jax.experimental.pallas import tpu as pltpu
from jax.sharding import PartitionSpec as P

F32 = jnp.float32
FULL = lax.Precision.HIGHEST
SB = 256
TR = 64
TC = 128
LANES = 128
CHUNK = 32
QS = 4
WS = 2
PER = QS // WS
LOT = 6
NARROW = 4
TILE = 512
LAST = 2
ORDER = (0, 2, 1, 3)


def _nn(a, b):
    return lax.dot_general(a, b, (((1,), (0,)), ((), ())), precision=FULL, preferred_element_type=F32)


def _nt(a, b):
    return lax.dot_general(a, b, (((1,), (1,)), ((), ())), precision=FULL, preferred_element_type=F32)


def _swap_middle(x0, x1):
    low = lax.broadcasted_iota(jnp.int32, x0.shape, 1) < LANES // 2
    half = LANES // 2
    return jnp.where(low, x0, pltpu.roll(x1, half, 1)), jnp.where(low, pltpu.roll(x0, half, 1), x1)


def _eliminate(left, right, first, count, group):
    rid = lax.broadcasted_iota(jnp.int32, (group, LANES), 0)
    lid = lax.broadcasted_iota(jnp.int32, (group, LANES), 1)
    here, under = [rid == j for j in range(group)], [rid > j for j in range(group)]
    diff = lid - rid
    upper, inverse = [], []
    for g in range(count // group):
        base = first + group * g
        top_l, top_r = left[:group], right[:group]
        cols = [jnp.broadcast_to(top_l[:, base + j : base + j + 1], (group, LANES)) for j in range(group)]
        scale, row_l, row_r, mult = [], [], [], {}
        for j in range(group):
            inv = lax.rsqrt(cols[j][j : j + 1])
            low = jnp.where(under[j], cols[j] * inv, 0.0)
            u_l, u_r = top_l[j : j + 1] * inv, top_r[j : j + 1] * inv
            for k in range(j + 1, group):
                mult[j, k] = cols[k][j : j + 1] * inv
                cols[k] = cols[k] - low * mult[j, k]
            top_l = jnp.where(here[j], u_l, top_l - low * u_l)
            top_r = jnp.where(here[j], u_r, top_r - low * u_r)
            scale.append(inv)
            row_l.append(u_l)
            row_r.append(u_r)
        upper.append(jnp.where(diff >= base, top_l, 0.0))
        inverse.append(top_r)
        rest = count - group * (g + 1)
        if rest == 0:
            break
        next_l, next_r = [], []
        for start in range(0, rest, CHUNK):
            stop = min(start + CHUNK, rest)
            a, b = left[group + start : group + stop], right[group + start : group + stop]
            below = [jnp.broadcast_to(a[:, base + j : base + j + 1], (stop - start, LANES)) for j in range(group)]
            for j in range(group):
                low = below[j] * scale[j]
                for k in range(j + 1, group):
                    below[k] = below[k] - low * mult[j, k]
                a = a - low * row_l[j]
                b = b - low * row_r[j]
            next_l.append(a)
            next_r.append(b)
        left = jnp.concatenate(next_l, 0) if len(next_l) > 1 else next_l[0]
        right = jnp.concatenate(next_r, 0) if len(next_r) > 1 else next_r[0]
    return upper, inverse


def _factor128(src, group, split):
    lane = lax.broadcasted_iota(jnp.int32, (LANES, LANES), 1)
    rows = lax.broadcasted_iota(jnp.int32, (LANES, LANES), 0)
    left, right = src, jnp.where(lane == rows, 1.0, 0.0).astype(F32)
    upper, inverse = [], []
    for first in range(0, LANES, split):
        u, w = _eliminate(left[:split], right[:split], first, split, group)
        upper += u
        inverse += w
        if first + split < LANES:
            u, w = jnp.concatenate(u, 0), jnp.concatenate(w, 0)
            t = u.T[first + split :]
            left, right = left[split:] - _nn(t, u), right[split:] - _nn(t, w)
    return upper, inverse


def _half(diag, upper, lower, inv, h, group, split):
    span = pl.ds(pl.multiple_of(LANES * h, LANES), LANES)
    u, w = _factor128(diag[span, span], group, split)
    for i in range(LANES // group):
        at = pl.ds(pl.multiple_of(LANES * h + group * i, group), group)
        upper[group * i : group * i + group, :] = u[i]
        inv[at, span] = w[i]
    lower[span, span] = upper[...].T


def _middle(diag, lower, inv):
    l10 = _nt(diag[LANES:, :LANES], inv[:LANES, :LANES])
    lower[LANES:, :LANES] = l10
    inv[LANES:, :LANES] = _nn(l10, inv[:LANES, :LANES])
    diag[LANES:, LANES:] = diag[LANES:, LANES:] - _nt(l10, l10)


def _inverse(lower, inv, invp):
    inv[LANES:, :LANES] = -_nn(inv[LANES:, LANES:], inv[LANES:, :LANES])
    inv[:LANES, LANES:] = jnp.zeros((LANES, LANES), F32)
    lower[:LANES, LANES:] = jnp.zeros((LANES, LANES), F32)
    for i in range(4):
        at = slice(TR * ORDER[i], TR * ORDER[i] + TR)
        s0, s1 = _swap_middle(inv[at, :LANES], inv[at, LANES:])
        invp[TR * i : TR * i + TR, :LANES] = s0
        invp[TR * i : TR * i + TR, LANES:] = s1


def _own_rows(lower, r):
    mine = pl.ds(pl.multiple_of(TR * r, TR), TR)
    return _swap_middle(lower[mine, :LANES], lower[mine, LANES:])


def _each(lo, hi, body):
    def step(i, carry):
        body(i)
        return carry

    lax.fori_loop(lo, hi, step, 0)


def _rows_of(q):
    return pl.ds(pl.multiple_of(QS * TR * q, QS * TR), QS * TR)


def _cols_of(k, n=1):
    return pl.ds(pl.multiple_of(TC * k, TC), n * TC)


def _kernel(steps, a_hbm, out_hbm, rest_hbm, mat, left, right, xl, yl, pieces, diag, upper, lower, inv, invp, a1, pair,
            load_sem, out_sem, sg_send, sg_recv, fw_send, fw_recv, f1_send, f1_recv, x_send, f2_recv, f3_send, f3_recv):
    r = lax.axis_index("row")
    c = lax.axis_index("col")
    x = r // 2
    p = r % 2
    me = r * 2 + c
    major = p == c
    minor = p != c
    chunks = steps // QS
    parts = steps // WS
    end = steps - LAST
    late = steps - 8
    rows, cols = steps * TR, steps * TC
    tiles = rows // TILE
    wide_u = max(u for u in range(2 * tiles) if sum(tiles - s // 2 for s in range(u, 2 * tiles)) > 4)
    own = pl.multiple_of(c * TC, TC)
    other = pl.multiple_of((1 - c) * TC, TC)
    xi = (r + 2) % 4
    y_peer = {"row": r, "col": 1 - c}
    x_peer = {"row": xi, "col": c}
    z_peer = {"row": xi, "col": 1 - c}
    d_peer = {"row": 2 * x + 1 - p, "col": c}
    peers = (d_peer, y_peer, x_peer, z_peer)
    each, rows_of, cols_of = _each, _rows_of, _cols_of

    def small(slot, i, n):
        ref = pieces.at[slot, me, pl.ds(0, n * TR)]
        return pltpu.make_async_remote_copy(ref, ref, sg_send.at[slot, i], sg_recv.at[slot, i], device_id=peers[i])

    sources = (None, r * 2 + 1 - c, xi * 2 + c, xi * 2 + 1 - c)

    def forward(slot, i, n):
        ref = pieces.at[slot, sources[i], pl.ds(0, n * TR)]
        return pltpu.make_async_remote_copy(ref, ref, fw_send.at[slot, i - 1], fw_recv.at[slot, i - 1], device_id=d_peer)

    def by_size(k, body):
        for n, chosen in ((2, k < late), (3, k >= late)):
            @pl.when(chosen)
            def _():
                body(n)

    def start_small(k):
        def body(n):
            for i in range(4):
                small((k + 3) % 3, i, n).start()

        by_size(k, body)

    def forward_small(k):
        def body(n):
            small((k + 3) % 3, 0, n).wait_recv()
            for i in range(1, 4):
                small((k + 3) % 3, i, n).wait_recv()
                forward((k + 3) % 3, i, n).start()

        by_size(k, body)

    def finish_small(k):
        def body(n):
            for i in range(1, 4):
                forward((k + 3) % 3, i, n).wait_recv()
            for i in range(4):
                small((k + 3) % 3, i, n).wait_send()
            for i in range(1, 4):
                forward((k + 3) % 3, i, n).wait_send()

        by_size(k, body)

    def f1(slot, w):
        ref = left.at[slot, pl.ds(WS * w, WS), :, pl.ds(own, TC)]
        return pltpu.make_async_remote_copy(ref, ref, f1_send.at[slot, w], f1_recv.at[slot, w], device_id=y_peer)

    def f2(slot, w, at):
        return pltpu.make_async_remote_copy(left.at[slot, pl.ds(WS * w, WS), :, pl.ds(at, TC)],
                                            right.at[slot, pl.ds(WS * w, WS), x, :, pl.ds(at, TC)],
                                            x_send.at[slot, w], f2_recv.at[slot, w], device_id=x_peer)

    def f3a(slot, w):
        return pltpu.make_async_remote_copy(left.at[slot, pl.ds(WS * w, WS)], right.at[slot, pl.ds(WS * w, WS), x],
                                            x_send.at[slot, w], f3_recv.at[slot, w], device_id=d_peer)

    def f3b(slot, w):
        ref = right.at[slot, pl.ds(WS * w, WS), 1 - x]
        return pltpu.make_async_remote_copy(ref, ref, f3_send.at[slot, w], f3_recv.at[slot, w], device_id=d_peer)

    def both_halves(slot, w):
        ref = right.at[slot, pl.ds(WS * w, WS), 1 - x]
        return pltpu.make_async_remote_copy(ref, ref, x_send.at[slot, w], f2_recv.at[slot, w], device_id=x_peer)

    def both_classes(slot, w):
        ref = right.at[slot, pl.ds(WS * w, WS)]
        return pltpu.make_async_remote_copy(ref, ref, x_send.at[slot, w], f3_recv.at[slot, w], device_id=d_peer)

    def relay(k, w):
        slot = k % 3
        f1(slot, w).wait_recv()

        @pl.when(major & (k < end - 1))
        def _():
            f2(slot, w, other).start()
            f3a(slot, w).start()
            right[slot, pl.ds(WS * w, WS), x] = left[slot, pl.ds(WS * w, WS)]

    def arrived(slot, w):
        both_halves(slot, w).wait_recv()

    def take(slot, w):
        both_classes(slot, w).wait_recv()

    def sent(slot, w):
        f1(slot, w).wait_send()

        @pl.when(major)
        def _():
            both_classes(slot, w).wait_send()

    head = min(3 * TC, cols)

    def load_first():
        return pltpu.make_async_copy(a_hbm.at[:TR, :TC], pieces.at[2, me, TR : 2 * TR], load_sem.at[chunks + 1])

    def load_head():
        return pltpu.make_async_copy(a_hbm.at[:, pl.ds(0, head)], mat.at[:, pl.ds(0, head)], load_sem.at[chunks])

    def load_rest(q):
        wide = min((QS * TC) * (q + 2), cols) - head
        at = (pl.ds(QS * TR * q, QS * TR), pl.ds(head, wide))
        return pltpu.make_async_copy(a_hbm.at[at], mat.at[at], load_sem.at[q])

    load_first().start()
    load_head().start()
    barrier = pltpu.get_barrier_semaphore()
    for peer in peers:
        pl.semaphore_signal(barrier, inc=1, device_id=peer)
    pieces[2, me, :TR] = jnp.zeros((TR, TC), F32)
    pieces[2, me, 2 * TR :] = jnp.zeros((TR, TC), F32)
    load_first().wait()
    pl.semaphore_wait(barrier, len(peers))
    start_small(-1)
    load_head().wait()
    for q in range(chunks):
        load_rest(q).start()

    def place_diag(slot):
        for i in range(4):
            s0, s1 = _swap_middle(pieces[slot, 2 * i, TR : 2 * TR, :], pieces[slot, 2 * i + 1, TR : 2 * TR, :])
            diag[TR * i : TR * i + TR, :LANES] = s0
            diag[TR * i : TR * i + TR, LANES:] = s1

    def place_next(slot):
        for i in range(4):
            a1[TR * i : TR * i + TR, :LANES] = pieces[slot, 2 * i, :TR, :]
            a1[TR * i : TR * i + TR, LANES:] = pieces[slot, 2 * i + 1, :TR, :]

    def stage(k, w):
        f1(k % 3, w).start()

    def stage_x(k, lot):
        @pl.when(major & (k < end - 1))
        def _():
            w0 = (k + 1) // WS
            cut = jnp.minimum(w0 + LOT, parts)
            each(jnp.where(lot == 0, w0, cut), jnp.where(lot == 0, cut, parts), lambda w: f2(k % 3, w, own).start())

    def stage_small(k):
        slot = k % 3
        one = pl.ds(pl.multiple_of(TR * (k + 1), TR), TR)
        two = pl.ds(pl.multiple_of(TR * jnp.minimum(k + 2, steps - 1), TR), TR)
        pieces[slot, me, :TR, :] = mat[one, cols_of(k)]
        pieces[slot, me, TR : 2 * TR, :] = mat[one, cols_of(k + 1)]
        pieces[slot, me, 2 * TR :, :] = mat[two, cols_of(k)]
        start_small(k)

    def first(q):
        left[0, pl.ds(QS * q, QS), :, pl.ds(own, TC)] = mat[rows_of(q), :TC].reshape(QS, TR, TC)

    each(0, chunks, first)
    stage(0, 0)
    stage(0, 1)
    stage_small(0)
    each(2, parts, lambda w: stage(0, w))
    stage_x(0, 0)
    forward_small(-1)
    finish_small(-1)
    place_diag(2)

    def step(k, carry):
        now = k % 3
        last = (k + 2) % 3
        q0 = k // QS
        w0 = (k + 1) // WS
        w1 = jnp.minimum((k + 2) // WS, parts - 1)

        u0 = (k + 2) // QS
        count = 0
        for u in range(2 * tiles):
            count = count + jnp.where(u >= u0, tiles - u // 2, 0)
        count = jnp.where(k > 0, count, 0)

        inner = 0
        for u in range(2 * tiles):
            inner = inner + jnp.where((u >= u0) & (u < u0 + 3), tiles - u // 2, 0)
        inner = jnp.minimum(inner, 8)

        def tile(i, among=count):
            u, past_of, total = 0, 0, 0
            for s in range(2 * tiles):
                total = total + jnp.where(s >= u0, tiles - s // 2, 0)
                past = i >= total
                u = u + jnp.where(past, 1, 0)
                past_of = jnp.where(past, total, past_of)
            live = i < among
            t = jnp.where(live, u // 2 + i - past_of, 0)
            seen = jnp.where(live, u, u0)
            u = jnp.where(live, u, 2 * tiles - 1)
            rs = pl.ds(pl.multiple_of(TILE * t, TILE), TILE)
            cs = pl.ds(pl.multiple_of(TILE * u, TILE), TILE)
            mat[rs, cs] = mat[rs, cs] - _nt(yl[rs, :], right[last, pl.ds(QS * seen, QS)].reshape(TILE, SB))

        lo = k // WS
        mid = jnp.minimum((k + 1) // WS + 1, parts)
        s1 = jnp.clip(PER * (u0 + 2), mid, parts)
        s2 = jnp.clip(PER * (u0 + 3), mid, parts)

        def pass_on(slot, a, b):
            def body(w):
                arrived(slot, w)
                f3b(slot, w).start()

            each(a, b, body)

        def finish_exchange(passed, taken):
            @pl.when((k > 0) & major)
            def _():
                pass_on(last, *passed)

            @pl.when((k > 0) & minor)
            def _():
                each(*taken, lambda w: take(last, w))

        def finish_pair(side):
            zero = jnp.zeros((2, 2, TR, SB), F32)

            @pl.when((k > 0) & side)
            def _():
                @pl.when((k <= late) & major)
                def _():
                    each(lo, mid, lambda w: f3b(last, w).wait_send())

                @pl.when((k > late) & major)
                def _():
                    each(lo, mid, lambda w: arrived(last, w))

                @pl.when((k > late) & minor)
                def _():
                    each(lo, mid, lambda w: take(last, w))

                right[last, pl.ds(k, 2)] = zero

                @pl.when((k > late) & major)
                def _():
                    each(lo, mid, lambda w: f3b(last, w).start())

        def relay_pair():
            @pl.when(k < late)
            def _():
                each(w0, w1 + 1, lambda w: relay(k, w))

            stage_x(k, 1)

        wide = (k > 0) & (u0 <= wide_u)

        @pl.when(wide)
        def _():
            finish_pair(True)
            finish_exchange((s1, s2), (mid, s1))

            @pl.when(k == 1)
            def _():
                for q in range(chunks):
                    load_rest(q).wait()

            def half(h):
                @pl.when(h == 1)
                def _():
                    _middle(diag, lower, inv)
                    finish_exchange((s2, parts), (s1, s2))

                for i in range(4):
                    tile(4 * h + i, inner)
                _half(diag, upper, lower, inv, h, 8, LANES)

                @pl.when(h == 0)
                def _():
                    relay_pair()

            each(0, 2, half)

        @pl.when(jnp.logical_not(wide))
        def _():
            finish_pair(major)
            finish_exchange((mid, parts), (mid, mid))
            _half(diag, upper, lower, inv, 0, 16, LANES // 2)
            relay_pair()
            finish_pair(minor)
            finish_exchange((mid, mid), (mid, parts))
            _middle(diag, lower, inv)

        @pl.when(jnp.logical_not(wide))
        def _():
            for i in range(NARROW):
                tile(i)
            _half(diag, upper, lower, inv, 1, 8, LANES)

        forward_small(k)

        @pl.when((k < late) & major)
        def _():
            def body(w):
                arrived(now, w)
                f3b(now, w).start()

            each(w0, w1 + 1, body)

        _inverse(lower, inv, invp)

        @pl.when(wide)
        def _():
            finish_exchange((mid, mid), (s2, parts))

        def put(q, at):
            return pltpu.make_async_copy(xl.at[rows_of(q), pl.ds(own, TC)], out_hbm.at[rows_of(q), cols_of(at)], out_sem.at[q])

        q1 = (k + 1) // QS
        q2 = jnp.minimum(q1 + 1, chunks - 1)
        inner = jnp.where(wide, inner, jnp.minimum(count, NARROW))
        over = count - inner
        extra = wide & (over > 0)
        over = jnp.where(extra, over - 1, over)
        upto = jnp.minimum(jnp.maximum(w0 + 5 + over // 2, PER * (q2 + 1)), parts)
        since = jnp.where(k < late, w1 + 1, w0)
        many = jnp.maximum(upto - since, 1)

        def share(j):
            return inner + (over * j) // many

        def between(j):
            each(share(j), share(j + 1), tile)

            @pl.when(since + j < upto)
            def _():
                relay(k, since + j)

        each(0, many, between)

        @pl.when(k > 0)
        def _():
            each(k // WS, parts, lambda w: sent(last, w))

            @pl.when(major)
            def _():
                each(jnp.where(k <= late, mid, lo), parts, lambda w: f3b(last, w).wait_send())

            each((k - 1) // QS, chunks, lambda q: put(q, k - 1).wait())

        def chunk_of(q):
            return left[now, pl.ds(QS * q, QS)].reshape(QS * TR, SB)

        def pair_of_pieces():
            for s in range(2):
                for h in range(2):
                    own_class = pieces.at[now, 2 * (c + 2 * s) + h]
                    pair[TR * s : TR * s + TR, TC * h : TC * h + TC] = own_class[:TR, :]
                    pair[TR * (2 + s) : TR * (2 + s) + TR, TC * h : TC * h + TC] = own_class[2 * TR :, :]

        finish_small(k)
        place_next(now)
        place_diag(now)

        @pl.when(k < late)
        def _():
            @pl.when(minor)
            def _():
                each(w0, w1 + 1, lambda w: take(now, w))

            pair[...] = right[now, pl.ds(k + 1, 2)].reshape(4 * TR, SB)

        @pl.when(k >= late)
        def _():
            pair_of_pieces()

        def begin():
            x1 = _nt(a1[...], invp[...])
            xa = _nt(chunk_of(q1), invp[...])
            xb = _nt(chunk_of(q2), invp[...])
            diag[...] = diag[...] - _nt(x1, x1)
            yl[rows_of(q1), :] = _nn(xa, invp[...])
            xl[rows_of(q1), :] = xa
            xl[rows_of(q2), :] = xb

        @pl.when(extra)
        def _():
            tile(count - 1)
            begin()

        @pl.when(jnp.logical_not(extra))
        def _():
            begin()

        cs = cols_of(k + 1, 2)
        slot = (k + 1) % 3

        def advance(q):
            qa, qb = jnp.minimum(q + 1, chunks - 1), jnp.minimum(q + 2, chunks - 1)
            each(jnp.maximum(upto, PER * (q + 2)), jnp.minimum(PER * (q + 3), parts), lambda w: relay(k, w))
            xb = _nt(chunk_of(qb), invp[...])
            ya = _nn(xl[rows_of(qa), :], invp[...])
            new = mat[rows_of(q), cs] - _nt(yl[rows_of(q), :], pair[...])
            mat[rows_of(q), cs] = new
            left[slot, pl.ds(QS * q, QS), :, pl.ds(own, TC)] = new[:, :TC].reshape(QS, TR, TC)
            yl[rows_of(qa), :] = ya
            xl[rows_of(qb), :] = xb

            for i in range(PER):
                @pl.when((k < end - 1) & (PER * q + i >= (k + 2) // WS))
                def _():
                    stage(k + 1, PER * q + i)

            @pl.when(q == jnp.minimum(k + 3, steps - 1) // QS)
            def _():
                stage_small(k + 1)

        each(q1, chunks, advance)
        stage_x(k + 1, 0)

        def clear_above(i):
            xl[pl.ds(pl.multiple_of(TR * i, TR), TR), :] = jnp.zeros((TR, SB), F32)

        each(QS * q0, k, clear_above)
        at = pl.ds(pl.multiple_of(TR * k, TR), TR)
        xl[at, :LANES], xl[at, LANES:] = _own_rows(lower, r)
        each(q0, chunks, lambda q: put(q, k).start())

        u1 = (k + 3) // QS
        next_mid = jnp.minimum((k + 2) // WS + 1, parts)

        @pl.when(major & (u1 <= wide_u))
        def _():
            pass_on(now, next_mid, jnp.clip(PER * (u1 + 2), next_mid, parts))
        return carry

    lax.fori_loop(0, end, step, 0)

    def leave(src, i):
        return pltpu.make_async_copy(src, rest_hbm.at[i], load_sem.at[i])

    slot = end % 3
    leave(diag, 0).start()
    forward_small(end)
    finish_small(end)
    place_next(slot)
    leave(a1, 1).start()
    for i in range(4):
        s0, s1 = _swap_middle(pieces[slot, 2 * i, TR : 2 * TR, :], pieces[slot, 2 * i + 1, TR : 2 * TR, :])
        pair[TR * i : TR * i + TR, :LANES] = s0
        pair[TR * i : TR * i + TR, LANES:] = s1
    leave(pair, 2).start()
    for i, src in enumerate((diag, a1, pair)):
        leave(src, i).wait()
    each((end - 1 + 1) // WS, parts, lambda w: f1((end - 1) % 3, w).wait_send())

    def drain(q):
        pltpu.make_async_copy(xl.at[rows_of(q), pl.ds(own, TC)], out_hbm.at[rows_of(q), cols_of(end - 1)], out_sem.at[q]).wait()

    each((end - 1) // QS, chunks, drain)


def _finish(steps, part_hbm, rest, out_hbm, buf, zeros, diag, upper, lower, inv, invp, in_sem, out_sem, zero_sem):
    r = lax.axis_index("row")
    c = lax.axis_index("col")
    chunks = steps // QS
    rows, cols = steps * TR, steps * TC
    kept = cols - LAST * TC
    own = pl.multiple_of(c * TC, TC)

    def block(q):
        return (pl.ds(QS * TR * q, QS * TR), pl.ds(0, min(QS * TC * (q + 1), kept)))

    def load(q):
        return pltpu.make_async_copy(part_hbm.at[block(q)], buf.at[block(q)], in_sem.at[q])

    def store(q):
        return pltpu.make_async_copy(buf.at[block(q)], out_hbm.at[block(q)], out_sem.at[q])

    def blank(q):
        wide = cols - QS * TC * (q + 1)
        return pltpu.make_async_copy(zeros.at[:, pl.ds(0, wide)],
                                     out_hbm.at[pl.ds(QS * TR * q, QS * TR), pl.ds(QS * TC * (q + 1), wide)], zero_sem.at[q])

    tail = (pl.ds(rows - QS * TR, QS * TR), pl.ds(kept, LAST * TC))
    final = pltpu.make_async_copy(buf.at[tail], out_hbm.at[tail], zero_sem.at[chunks - 1])

    for q in range(chunks):
        load(q).start()
    zeros[...] = jnp.zeros_like(zeros)
    buf[tail] = jnp.zeros((QS * TR, LAST * TC), F32)

    def own_half(s0, s1):
        return jnp.where(c == 0, s0, s1)

    diag[...] = rest[0]

    def rows_of_l(k):
        buf[rows - (LAST - k) * TR : rows - (LAST - k - 1) * TR, kept + k * TC : kept + k * TC + TC] = own_half(*_own_rows(lower, r))

    def half(i):
        h = i % 2

        @pl.when(h == 1)
        def _():
            _middle(diag, lower, inv)

        _half(diag, upper, lower, inv, h, 16, LANES // 2)

        @pl.when(i == 1)
        def _():
            for q in range(chunks):
                load(q).wait()
                store(q).start()
            for q in range(chunks - 1):
                blank(q).start()
            _inverse(lower, inv, invp)
            x1 = _nt(rest[1], invp[...])
            diag[...] = rest[2] - _nt(x1, x1)
            rows_of_l(0)
            invp[...] = x1
            mine = pl.ds(pl.multiple_of(TR * r, TR), TR)
            buf[rows - TR :, kept : kept + TC] = invp[mine, pl.ds(own, TC)]

        @pl.when(i == 3)
        def _():
            lower[:LANES, LANES:] = jnp.zeros((LANES, LANES), F32)
            rows_of_l(1)

    _each(0, 2 * LAST, half)
    final.start()
    for q in range(chunks):
        store(q).wait()
    for q in range(chunks - 1):
        blank(q).wait()
    final.wait()


def solution(mesh):
    def local_factor(blocks):
        row_blocks, block_size, local_cols = blocks.shape
        rows = row_blocks * block_size
        steps = local_cols // TC
        chunks, parts = steps // QS, steps // WS
        dma = pltpu.SemaphoreType.DMA
        vm = lambda *s: pltpu.VMEM(s, F32)
        anywhere = pl.BlockSpec(memory_space=pl.ANY)
        shape = jax.ShapeDtypeStruct((rows, local_cols), F32)
        part, rest = pl.pallas_call(
            lambda *refs: _kernel(steps, *refs),
            out_shape=(shape, jax.ShapeDtypeStruct((3, SB, SB), F32)),
            in_specs=[anywhere],
            out_specs=(anywhere, anywhere),
            scratch_shapes=[
                vm(rows, local_cols),
                vm(3, steps, TR, SB),
                vm(3, steps, 2, TR, SB),
                vm(rows, SB),
                vm(rows, SB),
                vm(3, 8, 3 * TR, TC),
                vm(SB, SB),
                vm(LANES, LANES),
                vm(SB, SB),
                vm(SB, SB),
                vm(SB, SB),
                vm(SB, SB),
                vm(SB, SB),
                dma((chunks + 2,)),
                dma((chunks,)),
                dma((3, 4)),
                dma((3, 4)),
                dma((3, 3)),
                dma((3, 3)),
                dma((3, parts)),
                dma((3, parts)),
                dma((3, parts)),
                dma((3, parts)),
                dma((3, parts)),
                dma((3, parts)),
            ],
            compiler_params=pltpu.CompilerParams(collective_id=0, has_side_effects=True, vmem_limit_bytes=67043328),
            name="factor",
        )(blocks.reshape(rows, local_cols))
        out = pl.pallas_call(
            lambda *refs: _finish(steps, *refs),
            out_shape=shape,
            in_specs=[anywhere, pl.BlockSpec(memory_space=pltpu.VMEM)],
            out_specs=anywhere,
            scratch_shapes=[
                vm(rows, local_cols),
                vm(QS * TR, local_cols - QS * TC),
                vm(SB, SB),
                vm(LANES, LANES),
                vm(SB, SB),
                vm(SB, SB),
                vm(SB, SB),
                dma((chunks,)),
                dma((chunks,)),
                dma((chunks,)),
            ],
            compiler_params=pltpu.CompilerParams(vmem_limit_bytes=60 * 2**20),
            name="finish",
        )(part, rest)
        return out.reshape(row_blocks, block_size, local_cols)

    spec = P(("part", "row"), None, "col")
    return jax.shard_map(local_factor, mesh=mesh, in_specs=(spec,), out_specs=spec, check_vma=False)
```

```python
import jax
import jax.numpy as jnp
from jax import lax
from jax.experimental import pallas as pl
from jax.experimental.pallas import tpu as pltpu
from jax.sharding import PartitionSpec as P

F32 = jnp.float32
FULL = lax.Precision.HIGHEST
SB = 256
TR = 64
TC = 128
LANES = 128
CHUNK = 32
QS = 4
WS = 2
PER = QS // WS
LOT = 6
NARROW = 4
TILE = 512
LAST = 2
ORDER = (0, 2, 1, 3)


def _nn(a, b):
    return lax.dot_general(a, b, (((1,), (0,)), ((), ())), precision=FULL, preferred_element_type=F32)


def _nt(a, b):
    return lax.dot_general(a, b, (((1,), (1,)), ((), ())), precision=FULL, preferred_element_type=F32)


def _swap_middle(x0, x1):
    low = lax.broadcasted_iota(jnp.int32, x0.shape, 1) < LANES // 2
    half = LANES // 2
    return jnp.where(low, x0, pltpu.roll(x1, half, 1)), jnp.where(low, pltpu.roll(x0, half, 1), x1)


def _eliminate(left, right, first, count, group):
    rid = lax.broadcasted_iota(jnp.int32, (group, LANES), 0)
    lid = lax.broadcasted_iota(jnp.int32, (group, LANES), 1)
    here, under = [rid == j for j in range(group)], [rid > j for j in range(group)]
    diff = lid - rid
    upper, inverse = [], []
    for g in range(count // group):
        base = first + group * g
        top_l, top_r = left[:group], right[:group]
        cols = [jnp.broadcast_to(top_l[:, base + j : base + j + 1], (group, LANES)) for j in range(group)]
        scale, row_l, row_r, mult = [], [], [], {}
        for j in range(group):
            inv = lax.rsqrt(cols[j][j : j + 1])
            low = jnp.where(under[j], cols[j] * inv, 0.0)
            u_l, u_r = top_l[j : j + 1] * inv, top_r[j : j + 1] * inv
            for k in range(j + 1, group):
                mult[j, k] = cols[k][j : j + 1] * inv
                cols[k] = cols[k] - low * mult[j, k]
            top_l = jnp.where(here[j], u_l, top_l - low * u_l)
            top_r = jnp.where(here[j], u_r, top_r - low * u_r)
            scale.append(inv)
            row_l.append(u_l)
            row_r.append(u_r)
        upper.append(jnp.where(diff >= base, top_l, 0.0))
        inverse.append(top_r)
        rest = count - group * (g + 1)
        if rest == 0:
            break
        next_l, next_r = [], []
        for start in range(0, rest, CHUNK):
            stop = min(start + CHUNK, rest)
            a, b = left[group + start : group + stop], right[group + start : group + stop]
            below = [jnp.broadcast_to(a[:, base + j : base + j + 1], (stop - start, LANES)) for j in range(group)]
            for j in range(group):
                low = below[j] * scale[j]
                for k in range(j + 1, group):
                    below[k] = below[k] - low * mult[j, k]
                a = a - low * row_l[j]
                b = b - low * row_r[j]
            next_l.append(a)
            next_r.append(b)
        left = jnp.concatenate(next_l, 0) if len(next_l) > 1 else next_l[0]
        right = jnp.concatenate(next_r, 0) if len(next_r) > 1 else next_r[0]
    return upper, inverse


def _factor128(src, group, split):
    lane = lax.broadcasted_iota(jnp.int32, (LANES, LANES), 1)
    rows = lax.broadcasted_iota(jnp.int32, (LANES, LANES), 0)
    left, right = src, jnp.where(lane == rows, 1.0, 0.0).astype(F32)
    upper, inverse = [], []
    for first in range(0, LANES, split):
        u, w = _eliminate(left[:split], right[:split], first, split, group)
        upper += u
        inverse += w
        if first + split < LANES:
            u, w = jnp.concatenate(u, 0), jnp.concatenate(w, 0)
            t = u.T[first + split :]
            left, right = left[split:] - _nn(t, u), right[split:] - _nn(t, w)
    return upper, inverse


def _half(diag, upper, lower, inv, h, group, split):
    span = pl.ds(pl.multiple_of(LANES * h, LANES), LANES)
    u, w = _factor128(diag[span, span], group, split)
    for i in range(LANES // group):
        at = pl.ds(pl.multiple_of(LANES * h + group * i, group), group)
        upper[group * i : group * i + group, :] = u[i]
        inv[at, span] = w[i]
    lower[span, span] = upper[...].T


def _middle(diag, lower, inv):
    l10 = _nt(diag[LANES:, :LANES], inv[:LANES, :LANES])
    lower[LANES:, :LANES] = l10
    inv[LANES:, :LANES] = _nn(l10, inv[:LANES, :LANES])
    diag[LANES:, LANES:] = diag[LANES:, LANES:] - _nt(l10, l10)


def _inverse(lower, inv, invp):
    inv[LANES:, :LANES] = -_nn(inv[LANES:, LANES:], inv[LANES:, :LANES])
    inv[:LANES, LANES:] = jnp.zeros((LANES, LANES), F32)
    lower[:LANES, LANES:] = jnp.zeros((LANES, LANES), F32)
    for i in range(4):
        at = slice(TR * ORDER[i], TR * ORDER[i] + TR)
        s0, s1 = _swap_middle(inv[at, :LANES], inv[at, LANES:])
        invp[TR * i : TR * i + TR, :LANES] = s0
        invp[TR * i : TR * i + TR, LANES:] = s1


def _own_rows(lower, r):
    mine = pl.ds(pl.multiple_of(TR * r, TR), TR)
    return _swap_middle(lower[mine, :LANES], lower[mine, LANES:])


def _each(lo, hi, body):
    def step(i, carry):
        body(i)
        return carry

    lax.fori_loop(lo, hi, step, 0)


def _rows_of(q):
    return pl.ds(pl.multiple_of(QS * TR * q, QS * TR), QS * TR)


def _cols_of(k, n=1):
    return pl.ds(pl.multiple_of(TC * k, TC), n * TC)


def _kernel(steps, a_hbm, out_hbm, rest_hbm, mat, left, right, xl, yl, pieces, diag, upper, lower, inv, invp, a1, pair,
            load_sem, out_sem, sg_send, sg_recv, fw_send, fw_recv, f1_send, f1_recv, x_send, f2_recv, f3_send, f3_recv):
    r = lax.axis_index("row")
    c = lax.axis_index("col")
    x = r // 2
    p = r % 2
    me = r * 2 + c
    major = p == c
    minor = p != c
    chunks = steps // QS
    parts = steps // WS
    end = steps - LAST
    late = steps - 8
    rows, cols = steps * TR, steps * TC
    tiles = rows // TILE
    wide_u = max(u for u in range(2 * tiles) if sum(tiles - s // 2 for s in range(u, 2 * tiles)) > 4)
    own = pl.multiple_of(c * TC, TC)
    other = pl.multiple_of((1 - c) * TC, TC)
    xi = (r + 2) % 4
    y_peer = {"row": r, "col": 1 - c}
    x_peer = {"row": xi, "col": c}
    z_peer = {"row": xi, "col": 1 - c}
    d_peer = {"row": 2 * x + 1 - p, "col": c}
    peers = (d_peer, y_peer, x_peer, z_peer)
    each, rows_of, cols_of = _each, _rows_of, _cols_of

    def small(slot, i, n):
        ref = pieces.at[slot, me, pl.ds(0, n * TR)]
        return pltpu.make_async_remote_copy(ref, ref, sg_send.at[slot, i], sg_recv.at[slot, i], device_id=peers[i])

    sources = (None, r * 2 + 1 - c, xi * 2 + c, xi * 2 + 1 - c)

    def forward(slot, i, n):
        ref = pieces.at[slot, sources[i], pl.ds(0, n * TR)]
        return pltpu.make_async_remote_copy(ref, ref, fw_send.at[slot, i - 1], fw_recv.at[slot, i - 1], device_id=d_peer)

    def by_size(k, body):
        if isinstance(k, int) and k < 0:
            body(1)
            return
        for n, chosen in ((2, (k < late) | (k == end)), (3, (k >= late) & (k != end))):
            @pl.when(chosen)
            def _():
                body(n)

    def start_small(k):
        def body(n):
            for i in range(4):
                small((k + 3) % 3, i, n).start()

        by_size(k, body)

    def forward_small(k):
        def body(n):
            small((k + 3) % 3, 0, n).wait_recv()
            for i in range(1, 4):
                small((k + 3) % 3, i, n).wait_recv()
                forward((k + 3) % 3, i, n).start()

        by_size(k, body)

    def finish_small(k):
        def body(n):
            for i in range(1, 4):
                forward((k + 3) % 3, i, n).wait_recv()
            for i in range(4):
                small((k + 3) % 3, i, n).wait_send()
            for i in range(1, 4):
                forward((k + 3) % 3, i, n).wait_send()

        by_size(k, body)

    def f1(slot, w):
        ref = left.at[slot, pl.ds(WS * w, WS), :, pl.ds(own, TC)]
        return pltpu.make_async_remote_copy(ref, ref, f1_send.at[slot, w], f1_recv.at[slot, w], device_id=y_peer)

    def f2(slot, w, at):
        return pltpu.make_async_remote_copy(left.at[slot, pl.ds(WS * w, WS), :, pl.ds(at, TC)],
                                            right.at[slot, pl.ds(WS * w, WS), x, :, pl.ds(at, TC)],
                                            x_send.at[slot, w], f2_recv.at[slot, w], device_id=x_peer)

    def f3a(slot, w):
        return pltpu.make_async_remote_copy(left.at[slot, pl.ds(WS * w, WS)], right.at[slot, pl.ds(WS * w, WS), x],
                                            x_send.at[slot, w], f3_recv.at[slot, w], device_id=d_peer)

    def f3b(slot, w):
        ref = right.at[slot, pl.ds(WS * w, WS), 1 - x]
        return pltpu.make_async_remote_copy(ref, ref, f3_send.at[slot, w], f3_recv.at[slot, w], device_id=d_peer)

    def both_halves(slot, w):
        ref = right.at[slot, pl.ds(WS * w, WS), 1 - x]
        return pltpu.make_async_remote_copy(ref, ref, x_send.at[slot, w], f2_recv.at[slot, w], device_id=x_peer)

    def both_classes(slot, w):
        ref = right.at[slot, pl.ds(WS * w, WS)]
        return pltpu.make_async_remote_copy(ref, ref, x_send.at[slot, w], f3_recv.at[slot, w], device_id=d_peer)

    def relay(k, w):
        slot = k % 3
        f1(slot, w).wait_recv()

        @pl.when(major & (k < end - 1))
        def _():
            f2(slot, w, other).start()
            f3a(slot, w).start()
            right[slot, pl.ds(WS * w, WS), x] = left[slot, pl.ds(WS * w, WS)]

    def arrived(slot, w):
        both_halves(slot, w).wait_recv()

    def take(slot, w):
        both_classes(slot, w).wait_recv()

    def sent(slot, w):
        f1(slot, w).wait_send()

        @pl.when(major)
        def _():
            both_classes(slot, w).wait_send()

    head = min(3 * TC, cols)

    def load_first():
        return pltpu.make_async_copy(a_hbm.at[:TR, :TC], pieces.at[2, me, :TR], load_sem.at[chunks + 1])

    def load_head():
        return pltpu.make_async_copy(a_hbm.at[:, pl.ds(0, head)], mat.at[:, pl.ds(0, head)], load_sem.at[chunks])

    def load_rest(q):
        wide = min((QS * TC) * (q + 2), cols) - head
        at = (pl.ds(QS * TR * q, QS * TR), pl.ds(head, wide))
        return pltpu.make_async_copy(a_hbm.at[at], mat.at[at], load_sem.at[q])

    load_first().start()
    load_head().start()
    barrier = pltpu.get_barrier_semaphore()
    for peer in peers:
        pl.semaphore_signal(barrier, inc=1, device_id=peer)
    load_first().wait()
    pl.semaphore_wait(barrier, len(peers))
    start_small(-1)
    load_head().wait()
    for q in range(chunks):
        load_rest(q).start()

    def place_diag(slot):
        for i in range(4):
            s0, s1 = _swap_middle(pieces[slot, 2 * i, :TR, :], pieces[slot, 2 * i + 1, :TR, :])
            diag[TR * i : TR * i + TR, :LANES] = s0
            diag[TR * i : TR * i + TR, LANES:] = s1

    def place_next(slot):
        for i in range(4):
            a1[TR * i : TR * i + TR, :LANES] = pieces[slot, 2 * i, TR : 2 * TR, :]
            a1[TR * i : TR * i + TR, LANES:] = pieces[slot, 2 * i + 1, TR : 2 * TR, :]

    def stage(k, w):
        f1(k % 3, w).start()

    def stage_x(k, lot):
        @pl.when(major & (k < end - 1))
        def _():
            w0 = (k + 1) // WS
            cut = jnp.minimum(w0 + LOT, parts)
            each(jnp.where(lot == 0, w0, cut), jnp.where(lot == 0, cut, parts), lambda w: f2(k % 3, w, own).start())

    def stage_small(k):
        slot = k % 3
        one = pl.ds(pl.multiple_of(TR * (k + 1), TR), TR)
        two = pl.ds(pl.multiple_of(TR * jnp.minimum(k + 2, steps - 1), TR), TR)
        pieces[slot, me, :TR, :] = mat[one, cols_of(k + 1)]
        pieces[slot, me, TR : 2 * TR, :] = mat[one, cols_of(k)]
        pieces[slot, me, 2 * TR :, :] = mat[two, cols_of(k)]
        start_small(k)

    def first(q):
        left[0, pl.ds(QS * q, QS), :, pl.ds(own, TC)] = mat[rows_of(q), :TC].reshape(QS, TR, TC)

    each(0, chunks, first)
    stage(0, 0)
    stage(0, 1)
    stage_small(0)
    each(2, parts, lambda w: stage(0, w))
    stage_x(0, 0)
    forward_small(-1)
    finish_small(-1)
    place_diag(2)

    def step(k, carry):
        now = k % 3
        last = (k + 2) % 3
        q0 = k // QS
        w0 = (k + 1) // WS
        w1 = jnp.minimum((k + 2) // WS, parts - 1)

        u0 = (k + 2) // QS
        count = 0
        for u in range(2 * tiles):
            count = count + jnp.where(u >= u0, tiles - u // 2, 0)
        count = jnp.where(k > 0, count, 0)

        inner = 0
        for u in range(2 * tiles):
            inner = inner + jnp.where((u >= u0) & (u < u0 + 3), tiles - u // 2, 0)
        inner = jnp.minimum(inner, 8)

        def tile(i, among=count):
            u, past_of, total = 0, 0, 0
            for s in range(2 * tiles):
                total = total + jnp.where(s >= u0, tiles - s // 2, 0)
                past = i >= total
                u = u + jnp.where(past, 1, 0)
                past_of = jnp.where(past, total, past_of)
            live = i < among
            t = jnp.where(live, u // 2 + i - past_of, 0)
            seen = jnp.where(live, u, u0)
            u = jnp.where(live, u, 2 * tiles - 1)
            rs = pl.ds(pl.multiple_of(TILE * t, TILE), TILE)
            cs = pl.ds(pl.multiple_of(TILE * u, TILE), TILE)
            mat[rs, cs] = mat[rs, cs] - _nt(yl[rs, :], right[last, pl.ds(QS * seen, QS)].reshape(TILE, SB))

        lo = k // WS
        mid = jnp.minimum((k + 1) // WS + 1, parts)
        s1 = jnp.clip(PER * (u0 + 2), mid, parts)
        s2 = jnp.clip(PER * (u0 + 3), mid, parts)

        def in_time(j):
            first = (j + 1) // QS
            return jnp.minimum(jnp.maximum((j + 1) // WS + 6, PER * (jnp.minimum(first + 1, chunks - 1) + 1)), parts)

        def pass_on(slot, a, b):
            def body(w):
                arrived(slot, w)
                f3b(slot, w).start()

            each(a, b, body)

        def finish_exchange(passed, taken):
            @pl.when((k > 0) & major)
            def _():
                pass_on(last, *passed)

            @pl.when((k > 0) & minor)
            def _():
                each(*taken, lambda w: take(last, w))

        def finish_pair(side):
            zero = jnp.zeros((2, 2, TR, SB), F32)

            @pl.when((k > 0) & side)
            def _():
                @pl.when((k <= late) & major)
                def _():
                    each(lo, mid, lambda w: f3b(last, w).wait_send())

                @pl.when((k > late) & major)
                def _():
                    each(lo, mid, lambda w: arrived(last, w))

                @pl.when((k > late) & minor)
                def _():
                    each(lo, mid, lambda w: take(last, w))

                right[last, pl.ds(k, 2)] = zero

                @pl.when((k > late) & major)
                def _():
                    each(lo, mid, lambda w: f3b(last, w).start())

        def relay_pair():
            @pl.when(k < late)
            def _():
                each(w0, w1 + 1, lambda w: relay(k, w))

            stage_x(k, 1)

        wide = (k > 0) & (u0 <= wide_u)

        @pl.when(wide)
        def _():
            finish_pair(True)
            finish_exchange((s1, s2), (mid, s1))

            @pl.when(k == 1)
            def _():
                for q in range(chunks):
                    load_rest(q).wait()

            def half(h):
                @pl.when(h == 1)
                def _():
                    _middle(diag, lower, inv)
                    finish_exchange((s2, parts), (s1, s2))

                for i in range(4):
                    tile(4 * h + i, inner)
                _half(diag, upper, lower, inv, h, 8, LANES)

                @pl.when(h == 0)
                def _():
                    relay_pair()

            each(0, 2, half)

        @pl.when(jnp.logical_not(wide))
        def _():
            sure = jnp.clip(in_time(k - 1), mid, parts)
            finish_pair(major)
            finish_exchange((mid, sure), (mid, mid))
            _half(diag, upper, lower, inv, 0, 16, LANES // 2)
            relay_pair()
            finish_pair(minor)
            finish_exchange((sure, parts), (mid, parts))
            _middle(diag, lower, inv)

        @pl.when(jnp.logical_not(wide))
        def _():
            for i in range(NARROW):
                tile(i)
            _half(diag, upper, lower, inv, 1, 8, LANES)

        forward_small(k)

        @pl.when((k < late) & major)
        def _():
            def body(w):
                arrived(now, w)
                f3b(now, w).start()

            each(w0, w1 + 1, body)

        _inverse(lower, inv, invp)

        @pl.when(wide)
        def _():
            finish_exchange((mid, mid), (s2, parts))

        def put(q, at):
            return pltpu.make_async_copy(xl.at[rows_of(q), pl.ds(own, TC)], out_hbm.at[rows_of(q), cols_of(at)], out_sem.at[q])

        q1 = (k + 1) // QS
        q2 = jnp.minimum(q1 + 1, chunks - 1)
        inner = jnp.where(wide, inner, jnp.minimum(count, NARROW))
        over = count - inner
        extra = wide & (over > 0)
        over = jnp.where(extra, over - 1, over)
        upto = jnp.minimum(jnp.maximum(w0 + 6 + over // 2, PER * (q2 + 1)), parts)
        since = jnp.where(k < late, w1 + 1, w0)
        many = jnp.maximum(upto - since, 1)

        def share(j):
            return inner + (over * j) // many

        def between(j):
            each(share(j), share(j + 1), tile)

            @pl.when(since + j < upto)
            def _():
                relay(k, since + j)

        each(0, many, between)

        @pl.when(k > 0)
        def _():
            each(k // WS, parts, lambda w: sent(last, w))

            @pl.when(major)
            def _():
                each(jnp.where(k <= late, mid, lo), parts, lambda w: f3b(last, w).wait_send())

            each((k - 1) // QS, chunks, lambda q: put(q, k - 1).wait())

        def chunk_of(q):
            return left[now, pl.ds(QS * q, QS)].reshape(QS * TR, SB)

        def pair_of_pieces():
            for s in range(2):
                for h in range(2):
                    own_class = pieces.at[now, 2 * (c + 2 * s) + h]
                    pair[TR * s : TR * s + TR, TC * h : TC * h + TC] = own_class[TR : 2 * TR, :]
                    pair[TR * (2 + s) : TR * (2 + s) + TR, TC * h : TC * h + TC] = own_class[2 * TR :, :]

        finish_small(k)
        place_next(now)
        place_diag(now)

        @pl.when(k < late)
        def _():
            @pl.when(minor)
            def _():
                each(w0, w1 + 1, lambda w: take(now, w))

            pair[...] = right[now, pl.ds(k + 1, 2)].reshape(4 * TR, SB)

        @pl.when(k >= late)
        def _():
            pair_of_pieces()

        def begin():
            x1 = _nt(a1[...], invp[...])
            xa = _nt(chunk_of(q1), invp[...])
            xb = _nt(chunk_of(q2), invp[...])
            diag[...] = diag[...] - _nt(x1, x1)
            yl[rows_of(q1), :] = _nn(xa, invp[...])
            xl[rows_of(q1), :] = xa
            xl[rows_of(q2), :] = xb

        @pl.when(extra)
        def _():
            tile(count - 1)
            begin()

        @pl.when(jnp.logical_not(extra))
        def _():
            begin()

        cs = cols_of(k + 1, 2)
        slot = (k + 1) % 3

        u1 = (k + 3) // QS
        next_mid = jnp.minimum((k + 2) // WS + 1, parts)
        next_sure = jnp.where(u1 <= wide_u, PER * (u1 + 2), 0)
        next_sure = jnp.clip(next_sure, next_mid, parts)

        def advance(q):
            qa, qb = jnp.minimum(q + 1, chunks - 1), jnp.minimum(q + 2, chunks - 1)
            each(jnp.maximum(upto, PER * (q + 2)), jnp.minimum(PER * (q + 3), parts), lambda w: relay(k, w))
            xb = _nt(chunk_of(qb), invp[...])
            ya = _nn(xl[rows_of(qa), :], invp[...])
            new = mat[rows_of(q), cs] - _nt(yl[rows_of(q), :], pair[...])
            mat[rows_of(q), cs] = new
            left[slot, pl.ds(QS * q, QS), :, pl.ds(own, TC)] = new[:, :TC].reshape(QS, TR, TC)
            yl[rows_of(qa), :] = ya
            xl[rows_of(qb), :] = xb

            @pl.when(major & (k < end - 1) & (q == jnp.maximum(q1, chunks - 2)))
            def _():
                pass_on(now, next_mid, next_sure)

            for i in range(PER):
                @pl.when((k < end - 1) & (PER * q + i >= (k + 2) // WS))
                def _():
                    stage(k + 1, PER * q + i)

            @pl.when(q == jnp.minimum(k + 3, steps - 1) // QS)
            def _():
                stage_small(k + 1)

        each(q1, chunks, advance)
        stage_x(k + 1, 0)

        def clear_above(i):
            xl[pl.ds(pl.multiple_of(TR * i, TR), TR), :] = jnp.zeros((TR, SB), F32)

        each(QS * q0, k, clear_above)
        at = pl.ds(pl.multiple_of(TR * k, TR), TR)
        xl[at, :LANES], xl[at, LANES:] = _own_rows(lower, r)
        each(q0, chunks, lambda q: put(q, k).start())
        return carry

    lax.fori_loop(0, end, step, 0)

    def leave(src, i):
        return pltpu.make_async_copy(src, rest_hbm.at[i], load_sem.at[i])

    slot = end % 3
    leave(diag, 0).start()
    forward_small(end)
    finish_small(end)
    place_next(slot)
    leave(a1, 1).start()
    for i in range(4):
        s0, s1 = _swap_middle(pieces[slot, 2 * i, :TR, :], pieces[slot, 2 * i + 1, :TR, :])
        pair[TR * i : TR * i + TR, :LANES] = s0
        pair[TR * i : TR * i + TR, LANES:] = s1
    leave(pair, 2).start()
    for i, src in enumerate((diag, a1, pair)):
        leave(src, i).wait()
    each((end - 1 + 1) // WS, parts, lambda w: f1((end - 1) % 3, w).wait_send())

    def drain(q):
        pltpu.make_async_copy(xl.at[rows_of(q), pl.ds(own, TC)], out_hbm.at[rows_of(q), cols_of(end - 1)], out_sem.at[q]).wait()

    each((end - 1) // QS, chunks, drain)


def _finish(steps, part_hbm, rest, out_hbm, buf, zeros, diag, upper, lower, inv, invp, in_sem, out_sem, zero_sem):
    r = lax.axis_index("row")
    c = lax.axis_index("col")
    chunks = steps // QS
    rows, cols = steps * TR, steps * TC
    kept = cols - LAST * TC
    own = pl.multiple_of(c * TC, TC)

    def block(q):
        return (pl.ds(QS * TR * q, QS * TR), pl.ds(0, min(QS * TC * (q + 1), kept)))

    def load(q):
        return pltpu.make_async_copy(part_hbm.at[block(q)], buf.at[block(q)], in_sem.at[q])

    def store(q):
        return pltpu.make_async_copy(buf.at[block(q)], out_hbm.at[block(q)], out_sem.at[q])

    def blank(q):
        wide = cols - QS * TC * (q + 1)
        return pltpu.make_async_copy(zeros.at[:, pl.ds(0, wide)],
                                     out_hbm.at[pl.ds(QS * TR * q, QS * TR), pl.ds(QS * TC * (q + 1), wide)], zero_sem.at[q])

    tail = (pl.ds(rows - QS * TR, QS * TR), pl.ds(kept, LAST * TC))
    final = pltpu.make_async_copy(buf.at[tail], out_hbm.at[tail], zero_sem.at[chunks - 1])

    for q in range(chunks):
        load(q).start()
    zeros[...] = jnp.zeros_like(zeros)
    buf[tail] = jnp.zeros((QS * TR, LAST * TC), F32)

    def own_half(s0, s1):
        return jnp.where(c == 0, s0, s1)

    diag[...] = rest[0]

    def rows_of_l(k):
        buf[rows - (LAST - k) * TR : rows - (LAST - k - 1) * TR, kept + k * TC : kept + k * TC + TC] = own_half(*_own_rows(lower, r))

    def half(i):
        h = i % 2

        @pl.when(h == 1)
        def _():
            _middle(diag, lower, inv)

        _half(diag, upper, lower, inv, h, 16, LANES // 2)

        @pl.when(i == 1)
        def _():
            for q in range(chunks):
                load(q).wait()
                store(q).start()
            for q in range(chunks - 1):
                blank(q).start()
            _inverse(lower, inv, invp)
            x1 = _nt(rest[1], invp[...])
            diag[...] = rest[2] - _nt(x1, x1)
            rows_of_l(0)
            invp[...] = x1
            mine = pl.ds(pl.multiple_of(TR * r, TR), TR)
            buf[rows - TR :, kept : kept + TC] = invp[mine, pl.ds(own, TC)]

        @pl.when(i == 3)
        def _():
            lower[:LANES, LANES:] = jnp.zeros((LANES, LANES), F32)
            rows_of_l(1)

    _each(0, 2 * LAST, half)
    final.start()
    for q in range(chunks):
        store(q).wait()
    for q in range(chunks - 1):
        blank(q).wait()
    final.wait()


def solution(mesh):
    def local_factor(blocks):
        row_blocks, block_size, local_cols = blocks.shape
        rows = row_blocks * block_size
        steps = local_cols // TC
        chunks, parts = steps // QS, steps // WS
        dma = pltpu.SemaphoreType.DMA
        vm = lambda *s: pltpu.VMEM(s, F32)
        anywhere = pl.BlockSpec(memory_space=pl.ANY)
        shape = jax.ShapeDtypeStruct((rows, local_cols), F32)
        part, rest = pl.pallas_call(
            lambda *refs: _kernel(steps, *refs),
            out_shape=(shape, jax.ShapeDtypeStruct((3, SB, SB), F32)),
            in_specs=[anywhere],
            out_specs=(anywhere, anywhere),
            scratch_shapes=[
                vm(rows, local_cols),
                vm(3, steps, TR, SB),
                vm(3, steps, 2, TR, SB),
                vm(rows, SB),
                vm(rows, SB),
                vm(3, 8, 3 * TR, TC),
                vm(SB, SB),
                vm(LANES, LANES),
                vm(SB, SB),
                vm(SB, SB),
                vm(SB, SB),
                vm(SB, SB),
                vm(SB, SB),
                dma((chunks + 2,)),
                dma((chunks,)),
                dma((3, 4)),
                dma((3, 4)),
                dma((3, 3)),
                dma((3, 3)),
                dma((3, parts)),
                dma((3, parts)),
                dma((3, parts)),
                dma((3, parts)),
                dma((3, parts)),
                dma((3, parts)),
            ],
            compiler_params=pltpu.CompilerParams(collective_id=0, has_side_effects=True, vmem_limit_bytes=67043328),
            name="factor",
        )(blocks.reshape(rows, local_cols))
        out = pl.pallas_call(
            lambda *refs: _finish(steps, *refs),
            out_shape=shape,
            in_specs=[anywhere, pl.BlockSpec(memory_space=pltpu.VMEM)],
            out_specs=anywhere,
            scratch_shapes=[
                vm(rows, local_cols),
                vm(QS * TR, local_cols - QS * TC),
                vm(SB, SB),
                vm(LANES, LANES),
                vm(SB, SB),
                vm(SB, SB),
                vm(SB, SB),
                dma((chunks,)),
                dma((chunks,)),
                dma((chunks,)),
            ],
            compiler_params=pltpu.CompilerParams(vmem_limit_bytes=60 * 2**20),
            name="finish",
        )(part, rest)
        return out.reshape(row_blocks, block_size, local_cols)

    spec = P(("part", "row"), None, "col")
    return jax.shard_map(local_factor, mesh=mesh, in_specs=(spec,), out_specs=spec, check_vma=False)
```

```python
import jax
import jax.numpy as jnp
from jax import lax
from jax.experimental import pallas as pl
from jax.experimental.pallas import tpu as pltpu
from jax.sharding import PartitionSpec as P

F32 = jnp.float32
FULL = lax.Precision.HIGHEST
SB = 256
TR = 64
TC = 128
LANES = 128
CHUNK = 32
QS = 4
WS = 2
PER = QS // WS
LOT = 6
NARROW = 2
TILE = 512
LAST = 2
ORDER = (0, 2, 1, 3)


def _nn(a, b):
    return lax.dot_general(a, b, (((1,), (0,)), ((), ())), precision=FULL, preferred_element_type=F32)


def _nt(a, b):
    return lax.dot_general(a, b, (((1,), (1,)), ((), ())), precision=FULL, preferred_element_type=F32)


def _swap_middle(x0, x1):
    low = lax.broadcasted_iota(jnp.int32, x0.shape, 1) < LANES // 2
    half = LANES // 2
    return jnp.where(low, x0, pltpu.roll(x1, half, 1)), jnp.where(low, pltpu.roll(x0, half, 1), x1)


def _eliminate(left, right, first, count, group):
    rid = lax.broadcasted_iota(jnp.int32, (group, LANES), 0)
    lid = lax.broadcasted_iota(jnp.int32, (group, LANES), 1)
    here, under = [rid == j for j in range(group)], [rid > j for j in range(group)]
    diff = lid - rid
    upper, inverse = [], []
    for g in range(count // group):
        base = first + group * g
        top_l, top_r = left[:group], right[:group]
        cols = [jnp.broadcast_to(top_l[:, base + j : base + j + 1], (group, LANES)) for j in range(group)]
        scale, row_l, row_r, mult = [], [], [], {}
        for j in range(group):
            inv = lax.rsqrt(cols[j][j : j + 1])
            low = jnp.where(under[j], cols[j] * inv, 0.0)
            u_l, u_r = top_l[j : j + 1] * inv, top_r[j : j + 1] * inv
            for k in range(j + 1, group):
                mult[j, k] = cols[k][j : j + 1] * inv
                cols[k] = cols[k] - low * mult[j, k]
            top_l = jnp.where(here[j], u_l, top_l - low * u_l)
            top_r = jnp.where(here[j], u_r, top_r - low * u_r)
            scale.append(inv)
            row_l.append(u_l)
            row_r.append(u_r)
        upper.append(jnp.where(diff >= base, top_l, 0.0))
        inverse.append(top_r)
        rest = count - group * (g + 1)
        if rest == 0:
            break
        next_l, next_r = [], []
        for start in range(0, rest, CHUNK):
            stop = min(start + CHUNK, rest)
            a, b = left[group + start : group + stop], right[group + start : group + stop]
            below = [jnp.broadcast_to(a[:, base + j : base + j + 1], (stop - start, LANES)) for j in range(group)]
            for j in range(group):
                low = below[j] * scale[j]
                for k in range(j + 1, group):
                    below[k] = below[k] - low * mult[j, k]
                a = a - low * row_l[j]
                b = b - low * row_r[j]
            next_l.append(a)
            next_r.append(b)
        left = jnp.concatenate(next_l, 0) if len(next_l) > 1 else next_l[0]
        right = jnp.concatenate(next_r, 0) if len(next_r) > 1 else next_r[0]
    return upper, inverse


def _factor128(src, group, split):
    lane = lax.broadcasted_iota(jnp.int32, (LANES, LANES), 1)
    rows = lax.broadcasted_iota(jnp.int32, (LANES, LANES), 0)
    left, right = src, jnp.where(lane == rows, 1.0, 0.0).astype(F32)
    upper, inverse = [], []
    for first in range(0, LANES, split):
        u, w = _eliminate(left[:split], right[:split], first, split, group)
        upper += u
        inverse += w
        if first + split < LANES:
            u, w = jnp.concatenate(u, 0), jnp.concatenate(w, 0)
            t = u.T[first + split :]
            left, right = left[split:] - _nn(t, u), right[split:] - _nn(t, w)
    return upper, inverse


def _half(diag, upper, lower, inv, h, group, split):
    span = pl.ds(pl.multiple_of(LANES * h, LANES), LANES)
    u, w = _factor128(diag[span, span], group, split)
    for i in range(LANES // group):
        at = pl.ds(pl.multiple_of(LANES * h + group * i, group), group)
        upper[group * i : group * i + group, :] = u[i]
        inv[at, span] = w[i]
    lower[span, span] = upper[...].T


def _middle(diag, lower, inv):
    l10 = _nt(diag[LANES:, :LANES], inv[:LANES, :LANES])
    lower[LANES:, :LANES] = l10
    inv[LANES:, :LANES] = _nn(l10, inv[:LANES, :LANES])
    diag[LANES:, LANES:] = diag[LANES:, LANES:] - _nt(l10, l10)


def _inverse(lower, inv, invp):
    inv[LANES:, :LANES] = -_nn(inv[LANES:, LANES:], inv[LANES:, :LANES])
    inv[:LANES, LANES:] = jnp.zeros((LANES, LANES), F32)
    lower[:LANES, LANES:] = jnp.zeros((LANES, LANES), F32)
    for i in range(4):
        at = slice(TR * ORDER[i], TR * ORDER[i] + TR)
        s0, s1 = _swap_middle(inv[at, :LANES], inv[at, LANES:])
        invp[TR * i : TR * i + TR, :LANES] = s0
        invp[TR * i : TR * i + TR, LANES:] = s1


def _own_rows(lower, r):
    mine = pl.ds(pl.multiple_of(TR * r, TR), TR)
    return _swap_middle(lower[mine, :LANES], lower[mine, LANES:])


def _each(lo, hi, body):
    def step(i, carry):
        body(i)
        return carry

    lax.fori_loop(lo, hi, step, 0)


def _rows_of(q):
    return pl.ds(pl.multiple_of(QS * TR * q, QS * TR), QS * TR)


def _cols_of(k, n=1):
    return pl.ds(pl.multiple_of(TC * k, TC), n * TC)


def _kernel(steps, a_hbm, out_hbm, rest_hbm, mat, left, right, xl, yl, pieces, diag, upper, lower, inv, invp, a1, pair,
            load_sem, out_sem, sg_send, sg_recv, fw_send, fw_recv, f1_send, f1_recv, x_send, f2_recv, f3_send, f3_recv):
    r = lax.axis_index("row")
    c = lax.axis_index("col")
    x = r // 2
    p = r % 2
    me = r * 2 + c
    major = p == c
    minor = p != c
    chunks = steps // QS
    parts = steps // WS
    end = steps - LAST
    late = steps - 10
    rows, cols = steps * TR, steps * TC
    tiles = rows // TILE
    wide_u = max(u for u in range(2 * tiles) if sum(tiles - s // 2 for s in range(u, 2 * tiles)) > 4)
    own = pl.multiple_of(c * TC, TC)
    other = pl.multiple_of((1 - c) * TC, TC)
    xi = (r + 2) % 4
    y_peer = {"row": r, "col": 1 - c}
    x_peer = {"row": xi, "col": c}
    z_peer = {"row": xi, "col": 1 - c}
    d_peer = {"row": 2 * x + 1 - p, "col": c}
    peers = (d_peer, y_peer, x_peer, z_peer)
    each, rows_of, cols_of = _each, _rows_of, _cols_of

    def small(slot, i, n):
        ref = pieces.at[slot, me, pl.ds(0, n * TR)]
        return pltpu.make_async_remote_copy(ref, ref, sg_send.at[slot, i], sg_recv.at[slot, i], device_id=peers[i])

    sources = (None, r * 2 + 1 - c, xi * 2 + c, xi * 2 + 1 - c)

    def forward(slot, i, n):
        ref = pieces.at[slot, sources[i], pl.ds(0, n * TR)]
        return pltpu.make_async_remote_copy(ref, ref, fw_send.at[slot, i - 1], fw_recv.at[slot, i - 1], device_id=d_peer)

    def by_size(k, body):
        if isinstance(k, int) and k < 0:
            body(1)
            return
        for n, chosen in ((2, (k < late) | (k == end)), (3, (k >= late) & (k != end))):
            @pl.when(chosen)
            def _():
                body(n)

    def start_small(k):
        def body(n):
            for i in range(4):
                small((k + 3) % 3, i, n).start()

        by_size(k, body)

    def forward_small(k):
        def body(n):
            small((k + 3) % 3, 0, n).wait_recv()
            for i in range(1, 4):
                small((k + 3) % 3, i, n).wait_recv()
                forward((k + 3) % 3, i, n).start()

        by_size(k, body)

    def finish_small(k):
        def body(n):
            for i in range(1, 4):
                forward((k + 3) % 3, i, n).wait_recv()
            for i in range(4):
                small((k + 3) % 3, i, n).wait_send()
            for i in range(1, 4):
                forward((k + 3) % 3, i, n).wait_send()

        by_size(k, body)

    def f1(slot, w):
        ref = left.at[slot, pl.ds(WS * w, WS), :, pl.ds(own, TC)]
        return pltpu.make_async_remote_copy(ref, ref, f1_send.at[slot, w], f1_recv.at[slot, w], device_id=y_peer)

    def f2(slot, w, at):
        return pltpu.make_async_remote_copy(left.at[slot, pl.ds(WS * w, WS), :, pl.ds(at, TC)],
                                            right.at[slot, pl.ds(WS * w, WS), x, :, pl.ds(at, TC)],
                                            x_send.at[slot, w], f2_recv.at[slot, w], device_id=x_peer)

    def f3a(slot, w):
        return pltpu.make_async_remote_copy(left.at[slot, pl.ds(WS * w, WS)], right.at[slot, pl.ds(WS * w, WS), x],
                                            x_send.at[slot, w], f3_recv.at[slot, w], device_id=d_peer)

    def f3b(slot, w):
        ref = right.at[slot, pl.ds(WS * w, WS), 1 - x]
        return pltpu.make_async_remote_copy(ref, ref, f3_send.at[slot, w], f3_recv.at[slot, w], device_id=d_peer)

    def both_halves(slot, w):
        ref = right.at[slot, pl.ds(WS * w, WS), 1 - x]
        return pltpu.make_async_remote_copy(ref, ref, x_send.at[slot, w], f2_recv.at[slot, w], device_id=x_peer)

    def both_classes(slot, w):
        ref = right.at[slot, pl.ds(WS * w, WS)]
        return pltpu.make_async_remote_copy(ref, ref, x_send.at[slot, w], f3_recv.at[slot, w], device_id=d_peer)

    def relay(k, w):
        slot = k % 3
        f1(slot, w).wait_recv()

        @pl.when(major & (k < end - 1))
        def _():
            f2(slot, w, other).start()
            f3a(slot, w).start()
            right[slot, pl.ds(WS * w, WS), x] = left[slot, pl.ds(WS * w, WS)]

    def arrived(slot, w):
        both_halves(slot, w).wait_recv()

    def take(slot, w):
        both_classes(slot, w).wait_recv()

    def sent(slot, w):
        f1(slot, w).wait_send()

        @pl.when(major)
        def _():
            both_classes(slot, w).wait_send()

    head = min(3 * TC, cols)

    def load_first():
        return pltpu.make_async_copy(a_hbm.at[:TR, :TC], pieces.at[2, me, :TR], load_sem.at[chunks + 1])

    def load_head():
        return pltpu.make_async_copy(a_hbm.at[:, pl.ds(0, head)], mat.at[:, pl.ds(0, head)], load_sem.at[chunks])

    def load_rest(q):
        wide = min((QS * TC) * (q + 2), cols) - head
        at = (pl.ds(QS * TR * q, QS * TR), pl.ds(head, wide))
        return pltpu.make_async_copy(a_hbm.at[at], mat.at[at], load_sem.at[q])

    load_first().start()
    load_head().start()
    barrier = pltpu.get_barrier_semaphore()
    for peer in peers:
        pl.semaphore_signal(barrier, inc=1, device_id=peer)
    load_first().wait()
    pl.semaphore_wait(barrier, len(peers))
    start_small(-1)
    load_head().wait()
    for q in range(chunks):
        load_rest(q).start()

    def place_diag(slot):
        for i in range(4):
            s0, s1 = _swap_middle(pieces[slot, 2 * i, :TR, :], pieces[slot, 2 * i + 1, :TR, :])
            diag[TR * i : TR * i + TR, :LANES] = s0
            diag[TR * i : TR * i + TR, LANES:] = s1

    def place_next(slot):
        for i in range(4):
            a1[TR * i : TR * i + TR, :LANES] = pieces[slot, 2 * i, TR : 2 * TR, :]
            a1[TR * i : TR * i + TR, LANES:] = pieces[slot, 2 * i + 1, TR : 2 * TR, :]

    def stage(k, w):
        f1(k % 3, w).start()

    def stage_x(k, lot):
        @pl.when(major & (k < end - 1))
        def _():
            w0 = (k + 1) // WS
            cut = jnp.minimum(w0 + LOT, parts)
            each(jnp.where(lot == 0, w0, cut), jnp.where(lot == 0, cut, parts), lambda w: f2(k % 3, w, own).start())

    def stage_small(k):
        slot = k % 3
        one = pl.ds(pl.multiple_of(TR * (k + 1), TR), TR)
        two = pl.ds(pl.multiple_of(TR * jnp.minimum(k + 2, steps - 1), TR), TR)
        pieces[slot, me, :TR, :] = mat[one, cols_of(k + 1)]
        pieces[slot, me, TR : 2 * TR, :] = mat[one, cols_of(k)]
        pieces[slot, me, 2 * TR :, :] = mat[two, cols_of(k)]
        start_small(k)

    def first(q):
        left[0, pl.ds(QS * q, QS), :, pl.ds(own, TC)] = mat[rows_of(q), :TC].reshape(QS, TR, TC)

    each(0, chunks, first)
    stage(0, 0)
    stage(0, 1)
    stage_small(0)
    each(2, parts, lambda w: stage(0, w))
    stage_x(0, 0)
    forward_small(-1)
    finish_small(-1)
    place_diag(2)

    def step(k, carry):
        now = k % 3
        last = (k + 2) % 3
        q0 = k // QS
        w0 = (k + 1) // WS
        w1 = jnp.minimum((k + 2) // WS, parts - 1)

        u0 = (k + 2) // QS
        count = 0
        for u in range(2 * tiles):
            count = count + jnp.where(u >= u0, tiles - u // 2, 0)
        count = jnp.where(k > 0, count, 0)

        inner = 0
        for u in range(2 * tiles):
            inner = inner + jnp.where((u >= u0) & (u < u0 + 3), tiles - u // 2, 0)
        rich = (k > 0) & (u0 <= min(1, wide_u - 3))
        inner = jnp.minimum(inner, jnp.where(rich, 10, 8))

        def tile(i, among=count):
            u, past_of, total = 0, 0, 0
            for s in range(2 * tiles):
                total = total + jnp.where(s >= u0, tiles - s // 2, 0)
                past = i >= total
                u = u + jnp.where(past, 1, 0)
                past_of = jnp.where(past, total, past_of)
            live = i < among
            t = jnp.where(live, u // 2 + i - past_of, 0)
            seen = jnp.where(live, u, u0)
            u = jnp.where(live, u, 2 * tiles - 1)
            rs = pl.ds(pl.multiple_of(TILE * t, TILE), TILE)
            cs = pl.ds(pl.multiple_of(TILE * u, TILE), TILE)
            mat[rs, cs] = mat[rs, cs] - _nt(yl[rs, :], right[last, pl.ds(QS * seen, QS)].reshape(TILE, SB))

        lo = k // WS
        mid = jnp.minimum((k + 1) // WS + 1, parts)
        s1 = jnp.clip(PER * (u0 + 2), mid, parts)
        s2 = jnp.clip(PER * (u0 + 3), mid, parts)

        def in_time(j):
            first = (j + 1) // QS
            return jnp.minimum(jnp.maximum((j + 1) // WS + 6, PER * (jnp.minimum(first + 1, chunks - 1) + 1)), parts)

        def pass_on(slot, a, b):
            def body(w):
                arrived(slot, w)
                f3b(slot, w).start()

            each(a, b, body)

        def finish_exchange(passed, taken):
            @pl.when((k > 0) & major)
            def _():
                pass_on(last, *passed)

            @pl.when((k > 0) & minor)
            def _():
                each(*taken, lambda w: take(last, w))

        def finish_pair(side):
            zero = jnp.zeros((2, 2, TR, SB), F32)

            @pl.when((k > 0) & side)
            def _():
                @pl.when((k <= late) & major)
                def _():
                    each(lo, mid, lambda w: f3b(last, w).wait_send())

                @pl.when((k > late) & major)
                def _():
                    each(lo, mid, lambda w: arrived(last, w))

                @pl.when((k > late) & minor)
                def _():
                    each(lo, mid, lambda w: take(last, w))

                right[last, pl.ds(k, 2)] = zero

                @pl.when((k > late) & major)
                def _():
                    each(lo, mid, lambda w: f3b(last, w).start())

        def relay_pair():
            @pl.when(k < late)
            def _():
                each(w0, w1 + 1, lambda w: relay(k, w))

            stage_x(k, 1)

        wide = (k > 0) & (u0 <= wide_u)

        @pl.when(wide)
        def _():
            finish_pair(True)
            finish_exchange((s1, s2), (mid, s1))

            @pl.when(k == 1)
            def _():
                for q in range(chunks):
                    load_rest(q).wait()

            def half(h):
                @pl.when(h == 1)
                def _():
                    finish_exchange((s2, parts), (s1, s2))

                    @pl.when(rich)
                    def _():
                        tile(8)
                        _middle(diag, lower, inv)

                    @pl.when(jnp.logical_not(rich))
                    def _():
                        _middle(diag, lower, inv)

                for i in range(4):
                    tile(4 * h + i, inner)
                _half(diag, upper, lower, inv, h, 8, LANES)

                @pl.when(h == 0)
                def _():
                    relay_pair()

            each(0, 2, half)

        @pl.when(jnp.logical_not(wide))
        def _():
            sure = jnp.clip(in_time(k - 1), mid, parts)
            finish_pair(major)
            finish_exchange((mid, sure), (mid, mid))
            _half(diag, upper, lower, inv, 0, 16, LANES // 2)
            relay_pair()
            finish_pair(minor)
            finish_exchange((sure, parts), (mid, parts))
            _middle(diag, lower, inv)

        @pl.when(jnp.logical_not(wide))
        def _():
            for i in range(NARROW):
                tile(i)
            _half(diag, upper, lower, inv, 1, 16, LANES // 2)

        forward_small(k)

        @pl.when((k < late) & major)
        def _():
            def body(w):
                arrived(now, w)
                f3b(now, w).start()

            each(w0, w1 + 1, body)

        @pl.when(rich)
        def _():
            tile(9)
            _inverse(lower, inv, invp)

        @pl.when(jnp.logical_not(rich))
        def _():
            _inverse(lower, inv, invp)

        @pl.when(wide)
        def _():
            finish_exchange((mid, mid), (s2, parts))

        def put(q, at):
            return pltpu.make_async_copy(xl.at[rows_of(q), pl.ds(own, TC)], out_hbm.at[rows_of(q), cols_of(at)], out_sem.at[q])

        q1 = (k + 1) // QS
        q2 = jnp.minimum(q1 + 1, chunks - 1)
        inner = jnp.where(wide, inner, jnp.minimum(count, NARROW))
        over = count - inner
        extra = wide & (over > 0)
        over = jnp.where(extra, over - 1, over)
        upto = jnp.minimum(jnp.maximum(w0 + 6 + over // 2, PER * (q2 + 1)), parts)
        since = jnp.where(k < late, w1 + 1, w0)
        many = jnp.maximum(upto - since, 1)

        def share(j):
            return inner + (over * j) // many

        def between(j):
            each(share(j), share(j + 1), tile)

            @pl.when(since + j < upto)
            def _():
                relay(k, since + j)

        each(0, many, between)

        @pl.when(k > 0)
        def _():
            each(k // WS, parts, lambda w: sent(last, w))

            @pl.when(major)
            def _():
                each(jnp.where(k <= late, mid, lo), parts, lambda w: f3b(last, w).wait_send())

            each((k - 1) // QS, chunks, lambda q: put(q, k - 1).wait())

        def chunk_of(q):
            return left[now, pl.ds(QS * q, QS)].reshape(QS * TR, SB)

        def pair_of_pieces():
            for s in range(2):
                for h in range(2):
                    own_class = pieces.at[now, 2 * (c + 2 * s) + h]
                    pair[TR * s : TR * s + TR, TC * h : TC * h + TC] = own_class[TR : 2 * TR, :]
                    pair[TR * (2 + s) : TR * (2 + s) + TR, TC * h : TC * h + TC] = own_class[2 * TR :, :]

        finish_small(k)
        place_next(now)
        place_diag(now)

        @pl.when(k < late)
        def _():
            @pl.when(minor)
            def _():
                each(w0, w1 + 1, lambda w: take(now, w))

            pair[...] = right[now, pl.ds(k + 1, 2)].reshape(4 * TR, SB)

        @pl.when(k >= late)
        def _():
            pair_of_pieces()

        def begin():
            x1 = _nt(a1[...], invp[...])
            xa = _nt(chunk_of(q1), invp[...])
            xb = _nt(chunk_of(q2), invp[...])
            diag[...] = diag[...] - _nt(x1, x1)
            yl[rows_of(q1), :] = _nn(xa, invp[...])
            xl[rows_of(q1), :] = xa
            xl[rows_of(q2), :] = xb

        @pl.when(extra)
        def _():
            tile(count - 1)
            begin()

        @pl.when(jnp.logical_not(extra))
        def _():
            begin()

        cs = cols_of(k + 1, 2)
        slot = (k + 1) % 3

        u1 = (k + 3) // QS
        next_mid = jnp.minimum((k + 2) // WS + 1, parts)
        next_sure = jnp.where(u1 <= wide_u, PER * (u1 + 2), 0)
        next_sure = jnp.clip(next_sure, next_mid, parts)

        def advance(q):
            qa, qb = jnp.minimum(q + 1, chunks - 1), jnp.minimum(q + 2, chunks - 1)
            each(jnp.maximum(upto, PER * (q + 2)), jnp.minimum(PER * (q + 3), parts), lambda w: relay(k, w))
            xb = _nt(chunk_of(qb), invp[...])
            ya = _nn(xl[rows_of(qa), :], invp[...])
            new = mat[rows_of(q), cs] - _nt(yl[rows_of(q), :], pair[...])
            mat[rows_of(q), cs] = new
            left[slot, pl.ds(QS * q, QS), :, pl.ds(own, TC)] = new[:, :TC].reshape(QS, TR, TC)
            yl[rows_of(qa), :] = ya
            xl[rows_of(qb), :] = xb

            @pl.when(major & (k < end - 1) & (q == jnp.maximum(q1, chunks - 2)))
            def _():
                pass_on(now, next_mid, next_sure)

            for i in range(PER):
                @pl.when((k < end - 1) & (PER * q + i >= (k + 2) // WS))
                def _():
                    stage(k + 1, PER * q + i)

            @pl.when(q == jnp.minimum(k + 3, steps - 1) // QS)
            def _():
                stage_small(k + 1)

        each(q1, chunks, advance)
        stage_x(k + 1, 0)

        def clear_above(i):
            xl[pl.ds(pl.multiple_of(TR * i, TR), TR), :] = jnp.zeros((TR, SB), F32)

        each(QS * q0, k, clear_above)
        at = pl.ds(pl.multiple_of(TR * k, TR), TR)
        xl[at, :LANES], xl[at, LANES:] = _own_rows(lower, r)
        each(q0, chunks, lambda q: put(q, k).start())
        return carry

    lax.fori_loop(0, end, step, 0)

    def leave(src, i):
        return pltpu.make_async_copy(src, rest_hbm.at[i], load_sem.at[i])

    slot = end % 3
    leave(diag, 0).start()
    forward_small(end)
    finish_small(end)
    place_next(slot)
    leave(a1, 1).start()
    for i in range(4):
        s0, s1 = _swap_middle(pieces[slot, 2 * i, :TR, :], pieces[slot, 2 * i + 1, :TR, :])
        pair[TR * i : TR * i + TR, :LANES] = s0
        pair[TR * i : TR * i + TR, LANES:] = s1
    leave(pair, 2).start()
    for i, src in enumerate((diag, a1, pair)):
        leave(src, i).wait()
    each((end - 1 + 1) // WS, parts, lambda w: f1((end - 1) % 3, w).wait_send())

    def drain(q):
        pltpu.make_async_copy(xl.at[rows_of(q), pl.ds(own, TC)], out_hbm.at[rows_of(q), cols_of(end - 1)], out_sem.at[q]).wait()

    each((end - 1) // QS, chunks, drain)


def _finish(steps, part_hbm, rest, out_hbm, buf, zeros, diag, upper, lower, inv, invp, in_sem, out_sem, zero_sem):
    r = lax.axis_index("row")
    c = lax.axis_index("col")
    chunks = steps // QS
    rows, cols = steps * TR, steps * TC
    kept = cols - LAST * TC
    own = pl.multiple_of(c * TC, TC)

    def block(q):
        return (pl.ds(QS * TR * q, QS * TR), pl.ds(0, min(QS * TC * (q + 1), kept)))

    def load(q):
        return pltpu.make_async_copy(part_hbm.at[block(q)], buf.at[block(q)], in_sem.at[q])

    def store(q):
        return pltpu.make_async_copy(buf.at[block(q)], out_hbm.at[block(q)], out_sem.at[q])

    def blank(q):
        wide = cols - QS * TC * (q + 1)
        return pltpu.make_async_copy(zeros.at[:, pl.ds(0, wide)],
                                     out_hbm.at[pl.ds(QS * TR * q, QS * TR), pl.ds(QS * TC * (q + 1), wide)], zero_sem.at[q])

    tail = (pl.ds(rows - QS * TR, QS * TR), pl.ds(kept, LAST * TC))
    final = pltpu.make_async_copy(buf.at[tail], out_hbm.at[tail], zero_sem.at[chunks - 1])

    for q in range(chunks):
        load(q).start()
    zeros[...] = jnp.zeros_like(zeros)
    buf[tail] = jnp.zeros((QS * TR, LAST * TC), F32)

    def own_half(s0, s1):
        return jnp.where(c == 0, s0, s1)

    diag[...] = rest[0]

    def rows_of_l(k):
        buf[rows - (LAST - k) * TR : rows - (LAST - k - 1) * TR, kept + k * TC : kept + k * TC + TC] = own_half(*_own_rows(lower, r))

    def half(i):
        h = i % 2

        @pl.when(h == 1)
        def _():
            _middle(diag, lower, inv)

        _half(diag, upper, lower, inv, h, 16, LANES // 2)

        @pl.when(i == 1)
        def _():
            for q in range(chunks):
                load(q).wait()
                store(q).start()
            for q in range(chunks - 1):
                blank(q).start()
            _inverse(lower, inv, invp)
            x1 = _nt(rest[1], invp[...])
            diag[...] = rest[2] - _nt(x1, x1)
            rows_of_l(0)
            invp[...] = x1
            mine = pl.ds(pl.multiple_of(TR * r, TR), TR)
            buf[rows - TR :, kept : kept + TC] = invp[mine, pl.ds(own, TC)]

        @pl.when(i == 3)
        def _():
            lower[:LANES, LANES:] = jnp.zeros((LANES, LANES), F32)
            rows_of_l(1)

    _each(0, 2 * LAST, half)
    final.start()
    for q in range(chunks):
        store(q).wait()
    for q in range(chunks - 1):
        blank(q).wait()
    final.wait()


def solution(mesh):
    def local_factor(blocks):
        row_blocks, block_size, local_cols = blocks.shape
        rows = row_blocks * block_size
        steps = local_cols // TC
        chunks, parts = steps // QS, steps // WS
        dma = pltpu.SemaphoreType.DMA
        vm = lambda *s: pltpu.VMEM(s, F32)
        anywhere = pl.BlockSpec(memory_space=pl.ANY)
        shape = jax.ShapeDtypeStruct((rows, local_cols), F32)
        part, rest = pl.pallas_call(
            lambda *refs: _kernel(steps, *refs),
            out_shape=(shape, jax.ShapeDtypeStruct((3, SB, SB), F32)),
            in_specs=[anywhere],
            out_specs=(anywhere, anywhere),
            scratch_shapes=[
                vm(rows, local_cols),
                vm(3, steps, TR, SB),
                vm(3, steps, 2, TR, SB),
                vm(rows, SB),
                vm(rows, SB),
                vm(3, 8, 3 * TR, TC),
                vm(SB, SB),
                vm(LANES, LANES),
                vm(SB, SB),
                vm(SB, SB),
                vm(SB, SB),
                vm(SB, SB),
                vm(SB, SB),
                dma((chunks + 2,)),
                dma((chunks,)),
                dma((3, 4)),
                dma((3, 4)),
                dma((3, 3)),
                dma((3, 3)),
                dma((3, parts)),
                dma((3, parts)),
                dma((3, parts)),
                dma((3, parts)),
                dma((3, parts)),
                dma((3, parts)),
            ],
            compiler_params=pltpu.CompilerParams(collective_id=0, has_side_effects=True, vmem_limit_bytes=67043328),
            name="factor",
        )(blocks.reshape(rows, local_cols))
        out = pl.pallas_call(
            lambda *refs: _finish(steps, *refs),
            out_shape=shape,
            in_specs=[anywhere, pl.BlockSpec(memory_space=pltpu.VMEM)],
            out_specs=anywhere,
            scratch_shapes=[
                vm(rows, local_cols),
                vm(QS * TR, local_cols - QS * TC),
                vm(SB, SB),
                vm(LANES, LANES),
                vm(SB, SB),
                vm(SB, SB),
                vm(SB, SB),
                dma((chunks,)),
                dma((chunks,)),
                dma((chunks,)),
            ],
            compiler_params=pltpu.CompilerParams(vmem_limit_bytes=60 * 2**20),
            name="finish",
        )(part, rest)
        return out.reshape(row_blocks, block_size, local_cols)

    spec = P(("part", "row"), None, "col")
    return jax.shard_map(local_factor, mesh=mesh, in_specs=(spec,), out_specs=spec, check_vma=False)
```
